16 devices in a mesh: dp: 1, tp: 16 (over x, y, z, core).
Axes of the slice: x: 2, y: 2, z: 2, core: 2. Of those that a mesh axis runs over, the one named last changes fastest.
Arguments:
- x: bfloat16 [3072, 6144], P(('dp', 'tp'))
- w: bfloat16 [6144, 32768], P(None, 'tp')
- label: int32 [3072], P(('dp', 'tp'))
Outputs:
- output 1: float32 [3072], P(('dp', 'tp'))
- output 2: bfloat16 [3072, 6144], P(('dp', 'tp'))
- output 3: bfloat16 [6144, 32768], P('dp', 'tp')
All inputs are finite; a program needn't handle non-finite values.
Results may differ from the reference program's by a relative error of at most 0.012.
Values are sent between devices in bfloat16 or wider.
A program may use at most 2 GiB of HBM per device.

```python
import jax
import jax.numpy as jnp

ROWS = 3072
D = 6144
VOCAB = 32768


def setup_inputs(seed: int = 0, part: int = 0) -> dict:
    kx, kw, kl = jax.random.split(jax.random.key(seed), 3)
    kx, kl = (jax.random.fold_in(k, part) for k in (kx, kl))
    return {
        "x": jax.random.normal(kx, (ROWS, D), jnp.float32).astype(jnp.bfloat16),
        "w": (jax.random.normal(kw, (D, VOCAB), jnp.float32) * (4.0 / D) ** 0.5).astype(jnp.bfloat16),
        "label": jax.random.randint(kl, (ROWS,), 0, VOCAB, jnp.int32),
    }


def reference(x, w, label):
    logits = jnp.dot(x, w, preferred_element_type=jnp.float32)
    top = jnp.max(logits, -1, keepdims=True)
    e = jnp.exp(logits - top)
    total = jnp.sum(e, -1, keepdims=True)
    hit = label[:, None] == jnp.arange(VOCAB, dtype=jnp.int32)[None, :]
    loss = jnp.log(total[:, 0]) + top[:, 0] - jnp.sum(jnp.where(hit, logits, 0.0), -1)
    by_logits = (e / total - hit.astype(jnp.float32)).astype(jnp.bfloat16)
    by_x = jnp.dot(by_logits, w.T, preferred_element_type=jnp.float32).astype(jnp.bfloat16)
    by_w = jnp.dot(x.T, by_logits, preferred_element_type=jnp.float32).astype(jnp.bfloat16)
    return loss, by_x, by_w
```

```python
import functools

import jax
import jax.numpy as jnp
from jax import lax
from jax.experimental import pallas as pl
from jax.experimental.pallas import tpu as pltpu
from jax.sharding import PartitionSpec as P

F32, BF16 = jnp.float32, jnp.bfloat16
VMEM_LIMIT = 60 * 1024 * 1024
CHUNKS = 4


def dot(a, b, contract):
    return lax.dot_general(a, b, (contract, ((), ())), preferred_element_type=F32)


def exchange_kernel(n, own_ref, all_ref, send_sems, recv_sems):
    me = lax.axis_index("tp")
    barrier = pltpu.get_barrier_semaphore()
    for j in range(1, n):
        pl.semaphore_signal(barrier, inc=1, device_id={"tp": lax.rem(me + j, n)}, device_id_type=pl.DeviceIdType.MESH)
    pl.semaphore_wait(barrier, n - 1)
    copies = []
    for j in range(1, n):
        copy = pltpu.make_async_remote_copy(
            src_ref=own_ref,
            dst_ref=all_ref.at[me],
            send_sem=send_sems.at[j],
            recv_sem=recv_sems.at[j],
            device_id={"tp": lax.rem(me + j, n)},
            device_id_type=pl.DeviceIdType.MESH,
        )
        copy.start()
        copies.append(copy)
    all_ref[me] = own_ref[...]
    for copy in copies:
        copy.wait()


def exchange(own, n, collective_id):
    return pl.pallas_call(
        functools.partial(exchange_kernel, n),
        out_shape=jax.ShapeDtypeStruct((n,) + own.shape, own.dtype),
        in_specs=[pl.BlockSpec(memory_space=pltpu.VMEM)],
        out_specs=pl.BlockSpec(memory_space=pltpu.VMEM),
        scratch_shapes=[pltpu.SemaphoreType.DMA((n,)), pltpu.SemaphoreType.DMA((n,))],
        compiler_params=pltpu.CompilerParams(collective_id=collective_id, has_side_effects=True),
        name="exchange",
    )(own)


def logits_kernel(x_ref, w_ref, lab_ref, z_ref, st_ref, m_s, s_s, r_s):
    j = pl.program_id(0)
    rows, wide = z_ref.shape
    block = 256

    @pl.when(j == 0)
    def _():
        m_s[...] = jnp.full(m_s.shape, -jnp.inf, F32)
        s_s[...] = jnp.zeros(s_s.shape, F32)
        r_s[...] = jnp.zeros(r_s.shape, F32)

    lane = lax.broadcasted_iota(jnp.int32, (block, 128), 1)
    for i in range(0, rows, block):
        part = slice(i, i + block)
        z = dot(x_ref[part, :], w_ref[...], ((1,), (0,)))
        z_ref[part, :] = z
        old = m_s[part, :]
        new = old
        for c in range(0, wide, 128):
            new = jnp.maximum(new, z[:, c : c + 128])
        total = s_s[part, :] * jnp.exp(old - new)
        right = r_s[part, :]
        off = lab_ref[part, :] - j * wide
        for c in range(0, wide, 128):
            total += jnp.exp(z[:, c : c + 128] - new)
            right += jnp.where(lane == off - c, z[:, c : c + 128], 0.0)
        m_s[part, :] = new
        s_s[part, :] = total
        r_s[part, :] = right

    @pl.when(j == pl.num_programs(0) - 1)
    def _():
        high = jnp.max(m_s[...], -1, keepdims=True)
        total = jnp.sum(s_s[...] * jnp.exp(m_s[...] - high), -1, keepdims=True)
        right = jnp.sum(r_s[...], -1, keepdims=True)
        at = lax.broadcasted_iota(jnp.int32, (rows, 128), 1)
        st_ref[...] = jnp.where(at == 0, high, jnp.where(at == 1, total, jnp.where(at == 2, right, 0.0))).T[:8, :]


def logits_call(x, w, lab):
    rows, depth = x.shape
    columns, wide = w.shape[1], 256
    return pl.pallas_call(
        logits_kernel,
        grid=(columns // wide,),
        in_specs=[
            pl.BlockSpec((rows, depth), lambda j: (0, 0)),
            pl.BlockSpec((depth, wide), lambda j: (0, j)),
            pl.BlockSpec((rows, 1), lambda j: (0, 0)),
        ],
        out_specs=[pl.BlockSpec((rows, wide), lambda j: (0, j)), pl.BlockSpec((8, rows), lambda j: (0, 0))],
        out_shape=[jax.ShapeDtypeStruct((rows, columns), F32), jax.ShapeDtypeStruct((8, rows), F32)],
        scratch_shapes=[pltpu.VMEM((rows, 128), F32)] * 3,
        compiler_params=pltpu.CompilerParams(vmem_limit_bytes=VMEM_LIMIT, dimension_semantics=("arbitrary",)),
        cost_estimate=pl.CostEstimate(
            flops=2 * rows * depth * columns, bytes_accessed=2 * depth * (rows + columns) + 4 * rows * columns, transcendentals=0
        ),
        name="logits",
    )(x, w, lab)


def by_x_kernel(z_ref, all_ref, lab_ref, w_ref, term_ref, g_ref, loss_ref, top_s, inv_s):
    j = pl.program_id(0)
    rows, columns = z_ref.shape
    block = 32

    @pl.when(j == 0)
    def _():
        own = all_ref[...]
        high, sums, right = own[:, 0, :], own[:, 1, :], own[:, 2, :]
        top = jnp.max(high, 0, keepdims=True)
        total = jnp.sum(sums * jnp.exp(high - top), 0, keepdims=True)
        loss_ref[...] = jnp.log(total) + top - jnp.sum(right, 0, keepdims=True)
        at = lax.broadcasted_iota(jnp.int32, (128, rows), 0)
        both = jnp.where(at == 0, top, jnp.where(at == 1, 1.0 / total, 0.0)).T
        top_s[...] = jnp.broadcast_to(both[:, 0:1], top_s.shape)
        inv_s[...] = jnp.broadcast_to(both[:, 1:2], inv_s.shape)
        lane = lax.broadcasted_iota(jnp.int32, (block, 128), 1)

        def body(i, carry):
            part = pl.ds(pl.multiple_of(i * block, block), block)
            top_b, inv_b = top_s[part, :], inv_s[part, :]
            off = jnp.broadcast_to(lab_ref[part, :], (block, 128)) - lane
            for c in range(0, columns, 128):
                e = jnp.exp(z_ref[part, c : c + 128] - top_b) * inv_b
                g_ref[part, c : c + 128] = jnp.where(off == c, e - 1.0, e).astype(BF16)
            return carry

        lax.fori_loop(0, rows // block, body, 0)

    term_ref[...] = dot(g_ref[...], w_ref[...], ((1,), (1,))).astype(BF16)


def by_x_call(z, all_stats, lab, w):
    rows, columns = z.shape
    depth, tall = w.shape[0], 512
    n = all_stats.shape[0]
    return pl.pallas_call(
        by_x_kernel,
        grid=(depth // tall,),
        in_specs=[
            pl.BlockSpec((rows, columns), lambda j: (0, 0)),
            pl.BlockSpec((n, 8, rows), lambda j: (0, 0, 0)),
            pl.BlockSpec((rows, 1), lambda j: (0, 0)),
            pl.BlockSpec((tall, columns), lambda j: (j, 0)),
        ],
        out_specs=[
            pl.BlockSpec((rows, tall), lambda j: (0, j)),
            pl.BlockSpec((rows, columns), lambda j: (0, 0)),
            pl.BlockSpec((1, rows), lambda j: (0, 0)),
        ],
        out_shape=[
            jax.ShapeDtypeStruct((rows, depth), BF16),
            jax.ShapeDtypeStruct((rows, columns), BF16),
            jax.ShapeDtypeStruct((1, rows), F32),
        ],
        scratch_shapes=[pltpu.VMEM((rows, 128), F32)] * 2,
        compiler_params=pltpu.CompilerParams(vmem_limit_bytes=VMEM_LIMIT, dimension_semantics=("arbitrary",)),
        cost_estimate=pl.CostEstimate(
            flops=2 * rows * depth * columns, bytes_accessed=2 * depth * (rows + columns) + 6 * rows * columns, transcendentals=0
        ),
        name="by_x",
    )(z, all_stats, lab, w)


def by_w_kernel(k, *refs):
    x_refs, g_refs, out_ref = refs[:k], refs[k : 2 * k], refs[2 * k]
    acc = None
    for x_ref, g_ref in zip(x_refs, g_refs):
        part = dot(x_ref[...], g_ref[...], ((0,), (0,)))
        acc = part if acc is None else acc + part
    out_ref[...] = acc.astype(BF16)


def by_w_call(xs, gs):
    k = len(xs)
    rows, depth = xs[0].shape
    columns, tall = gs[0].shape[1], 256
    return pl.pallas_call(
        functools.partial(by_w_kernel, k),
        grid=(depth // tall,),
        in_specs=[pl.BlockSpec((rows, tall), lambda j: (0, j))] * k + [pl.BlockSpec((rows, columns), lambda j: (0, 0))] * k,
        out_specs=pl.BlockSpec((tall, columns), lambda j: (j, 0)),
        out_shape=jax.ShapeDtypeStruct((depth, columns), BF16),
        compiler_params=pltpu.CompilerParams(vmem_limit_bytes=VMEM_LIMIT, dimension_semantics=("arbitrary",)),
        cost_estimate=pl.CostEstimate(
            flops=2 * k * rows * depth * columns,
            bytes_accessed=2 * k * rows * (depth + columns) + 2 * depth * columns,
            transcendentals=0,
        ),
        name="by_w",
    )(*xs, *gs)


def solution(mesh):
    n = mesh.shape["tp"]

    def step(x, w, label):
        me, own_rows, columns = lax.axis_index("tp"), x.shape[0], w.shape[1]
        r = own_rows // CHUNKS
        xs = [lax.all_gather(x[c * r : (c + 1) * r], "tp", axis=0, tiled=True) for c in range(CHUNKS)]
        padded = jnp.pad(label.reshape(1, own_rows), ((0, 0), (0, -own_rows % 128)))
        wanted = exchange(padded, n, 0)[:, 0, :own_rows].reshape(n, CHUNKS, r) - me * columns
        gs, terms, losses = [], [], []
        for c in range(CHUNKS):
            lab = wanted[:, c, :].reshape(n * r, 1)
            z, own = logits_call(xs[c], w, lab)
            all_stats = exchange(own, n, 1 + c)
            term, g, loss = by_x_call(z, all_stats, lab, w)
            terms.append(lax.psum_scatter(term, "tp", scatter_dimension=0, tiled=True))
            gs.append(g)
            losses.append(lax.dynamic_slice_in_dim(loss, me * r, r, 1)[0])
        by_w = by_w_call(xs, gs)
        return jnp.concatenate(losses), jnp.concatenate(terms), by_w

    return jax.shard_map(
        step,
        mesh=mesh,
        in_specs=(P(("dp", "tp"), None), P(None, "tp"), P(("dp", "tp"))),
        out_specs=(P(("dp", "tp")), P(("dp", "tp"), None), P("dp", "tp")),
        check_vma=False,
    )
```

```python
import functools

import jax
import jax.numpy as jnp
from jax import lax
from jax.experimental import pallas as pl
from jax.experimental.pallas import tpu as pltpu
from jax.sharding import PartitionSpec as P

F32, BF16 = jnp.float32, jnp.bfloat16
MESH = pl.DeviceIdType.MESH
VMEM_LIMIT = 63 * 1024 * 1024

ORDERS = ((4, 2, 1), (2, 1, 4), (1, 4, 2))
MASKS = tuple((0, a, b, c, a | b, a | c, b | c, a | b | c) for a, b, c in ORDERS)
LAST = (None, 0, 1, 2, 1, 2, 2, 2)
BEFORE = (None, 0, 0, 0, 1, 1, 2, 4)
BATCHES, PIECES = 8, 3
BY_W_TALL = 256
BY_W_EARLY = 10


def dot(a, b, contract):
    return lax.dot_general(a, b, (contract, ((), ())), preferred_element_type=F32)


def flip(index, mask):
    for bit in (1, 2, 4, 8):
        if mask & bit:
            index = index + bit - 2 * bit * lax.rem(lax.div(index, bit), 2)
    return index


def across(me, i, k):
    return {"tp": flip(me, 2 * ORDERS[i][LAST[k]])}


def meet(n, me):
    barrier = pltpu.get_barrier_semaphore()
    for j in range(1, n):
        pl.semaphore_signal(barrier, inc=1, device_id={"tp": lax.rem(me + j, n)}, device_id_type=MESH)
    pl.semaphore_wait(barrier, n - 1)


def to_all(n, me, own_ref, all_ref, send_sems, recv_sems):
    copies = []
    for j in range(1, n):
        copies.append(
            pltpu.make_async_remote_copy(
                src_ref=own_ref,
                dst_ref=all_ref.at[me],
                send_sem=send_sems.at[j],
                recv_sem=recv_sems.at[j],
                device_id={"tp": lax.rem(me + j, n)},
                device_id_type=MESH,
            )
        )
    for copy in copies:
        copy.start()
    return copies


def as_column(row):
    return jnp.broadcast_to(row, (128, 128)).T


def logits_kernel(
    n, x_ref, w_ref, lab_ref, xb_ref, z_ref, labs_ref, top_ref, inv_ref, loss_ref,
    w_v, x_v, z_v, m_s, s_s, r_s, off_s, st_s, own_s, all_s,
    w_sem, x_sem, keep_sem, z_sem, ici_send, ici_recv, pair_send, pair_recv, lab_send, lab_recv, st_send, st_recv,
):
    me = lax.axis_index("tp")
    core = lax.rem(me, 2)
    piece = x_ref.shape[0] // PIECES
    half = PIECES * piece
    depth, columns = w_ref.shape
    wide = 256

    w_parts = 8
    w_copies = []
    for p in range(w_parts):
        part = pl.ds(p * (depth // w_parts), depth // w_parts)
        w_copies.append(pltpu.make_async_copy(w_ref.at[part], w_v.at[part], w_sem.at[p]))
        w_copies[-1].start()
    x_load = pltpu.make_async_copy(x_ref, x_v.at[0], x_sem.at[0, 0])
    x_load.start()

    meet(n, me)

    def slot(k, i, other):
        return xb_ref.at[k, pl.ds(i * 2 * piece + other * piece, piece)]

    def source(k, i):
        return x_ref.at[pl.ds(i * piece, piece)] if k == 0 else slot(k, i, 0)

    sent = {}

    def send(k, i):
        sent["ici", k, i] = pltpu.make_async_remote_copy(
            src_ref=source(BEFORE[k], i),
            dst_ref=slot(k, i, 0),
            send_sem=ici_send.at[k, i],
            recv_sem=ici_recv.at[k, i],
            device_id=across(me, i, k),
            device_id_type=MESH,
        )
        sent["ici", k, i].start()

    def share(k, i):
        sent["pair", k, i] = pltpu.make_async_remote_copy(
            src_ref=source(k, i),
            dst_ref=slot(k, i, 1),
            send_sem=pair_send.at[k, i],
            recv_sem=pair_recv.at[k, i],
            device_id={"tp": flip(me, 1)},
            device_id_type=MESH,
        )
        sent["pair", k, i].start()

    labels = to_all(n, me, lab_ref, labs_ref, lab_send, lab_recv)
    for i in range(PIECES):
        send(1, i)
    for i in range(PIECES):
        share(0, i)
    for k in (2, 3):
        for i in range(PIECES):
            send(k, i)
    labs_ref[me] = lab_ref[...]
    x_load.wait()
    kept = []
    for i in range(PIECES):
        kept.append(pltpu.make_async_copy(x_v.at[0, pl.ds(i * piece, piece)], slot(0, i, 0), keep_sem.at[i]))
        kept[-1].start()
    for copy in labels:
        copy.wait_recv()
    for copy in w_copies:
        copy.wait()

    z_copies = {0: [], 1: []}
    lane = lax.broadcasted_iota(jnp.int32, (half, 128), 1)

    def compute(k, other):
        for i in range(PIECES):
            dev = flip(me, 2 * MASKS[i][k] + other)
            row = (labs_ref[dev, pl.ds(i, 1), :] - me * columns).astype(F32)
            off_s[pl.ds(i * piece, piece), :] = as_column(row)[:piece].astype(jnp.int32)
        m_s[...] = jnp.full(m_s.shape, -jnp.inf, F32)
        s_s[...] = jnp.zeros(s_s.shape, F32)
        r_s[...] = jnp.zeros(r_s.shape, F32)
        for copy in z_copies[other]:
            copy.wait()

        def body(j, carry):
            at = pl.multiple_of(j * wide, wide)
            z = dot(x_v[other], w_v[:, pl.ds(at, wide)], ((1,), (0,)))
            z_v[other, :, pl.ds(at, wide)] = z
            old = m_s[...]
            new = old
            for c in range(0, wide, 128):
                new = jnp.maximum(new, z[:, c : c + 128])
            total = s_s[...] * jnp.exp(old - new)
            right = r_s[...]
            off = off_s[...] - at
            for c in range(0, wide, 128):
                total += jnp.exp(z[:, c : c + 128] - new)
                right += jnp.where(lane == off - c, z[:, c : c + 128], 0.0)
            m_s[...] = new
            s_s[...] = total
            r_s[...] = right
            return carry

        lax.fori_loop(0, columns // wide, body, 0)
        z_copies[other] = []
        for i in range(PIECES):
            z_copies[other].append(
                pltpu.make_async_copy(
                    z_v.at[other, pl.ds(i * piece, piece)],
                    z_ref.at[k, pl.ds(i * 2 * piece + other * piece, piece)],
                    z_sem.at[other, i],
                )
            )
            z_copies[other][-1].start()
        high = jnp.max(m_s[...], -1, keepdims=True)
        total = jnp.sum(s_s[...] * jnp.exp(m_s[...] - high), -1, keepdims=True)
        right = jnp.sum(r_s[...], -1, keepdims=True)
        st_s[other] = jnp.where(lane == 0, high, jnp.where(lane == 1, total, jnp.where(lane == 2, right, 0.0)))

    def load(k, other):
        copies = []
        for i in range(PIECES):
            copies.append(pltpu.make_async_copy(slot(k, i, other), x_v.at[other, pl.ds(i * piece, piece)], x_sem.at[other, i]))
            copies[-1].start()
        return copies

    for k in range(BATCHES):
        if k > 0:
            for i in range(PIECES):
                sent["ici", k, i].wait_recv()
            for i in range(PIECES):
                for later in range(4, BATCHES):
                    if BEFORE[later] == k:
                        send(later, i)
                share(k, i)
            for copy in load(k, 0):
                copy.wait()
        compute(k, 0)
        for i in range(PIECES):
            sent["pair", k, i].wait_recv()
        if k == 0:
            for copy in kept:
                copy.wait()
        for copy in load(k, 1):
            copy.wait()
        compute(k, 1)
        for i in range(PIECES):
            part = pl.ds(i * piece, piece)
            first, second = st_s[0, part, :], st_s[1, part, :]
            both = jnp.concatenate(
                [jnp.where(core == 0, first, second), jnp.where(core == 0, second, first)], 0
            ).T
            pair = lax.div(flip(me, 2 * MASKS[i][k]), 2) * PIECES + i
            for t in range(3):
                own_s[t, pl.ds(pair, 1), :] = both[t : t + 1, :]

    stats = to_all(n, me, own_s, all_s, st_send, st_recv)
    all_s[me] = own_s[...]
    for copy in stats:
        copy.wait_recv()
    high, sums, right = all_s[:, 0], all_s[:, 1], all_s[:, 2]
    top = jnp.max(high, 0)
    total = jnp.sum(sums * jnp.exp(high - top[None]), 0)
    top_ref[...] = top
    inv_ref[...] = 1.0 / total
    loss_ref[...] = jnp.log(total) + top - jnp.sum(right, 0)
    for copy in labels + stats + list(sent.values()):
        copy.wait_send()
    for copies in z_copies.values():
        for copy in copies:
            copy.wait()


def logits_call(n, x, w, lab):
    own, depth = x.shape
    columns = w.shape[1]
    pairs = n // 2 * PIECES
    anywhere, vmem = pl.BlockSpec(memory_space=pl.ANY), pl.BlockSpec(memory_space=pltpu.VMEM)
    dma = pltpu.SemaphoreType.DMA
    return pl.pallas_call(
        functools.partial(logits_kernel, n),
        in_specs=[anywhere, anywhere, vmem],
        out_specs=[anywhere, anywhere, vmem, vmem, vmem, vmem],
        out_shape=[
            jax.ShapeDtypeStruct((BATCHES, 2 * own, depth), BF16),
            jax.ShapeDtypeStruct((BATCHES, 2 * own, columns), F32),
            jax.ShapeDtypeStruct((n,) + lab.shape, jnp.int32),
            jax.ShapeDtypeStruct((pairs, 128), F32),
            jax.ShapeDtypeStruct((pairs, 128), F32),
            jax.ShapeDtypeStruct((pairs, 128), F32),
        ],
        scratch_shapes=[
            pltpu.VMEM((depth, columns), BF16),
            pltpu.VMEM((2, own, depth), BF16),
            pltpu.VMEM((2, own, columns), F32),
            pltpu.VMEM((own, 128), F32),
            pltpu.VMEM((own, 128), F32),
            pltpu.VMEM((own, 128), F32),
            pltpu.VMEM((own, 128), jnp.int32),
            pltpu.VMEM((2, own, 128), F32),
            pltpu.VMEM((3, pairs, 128), F32),
            pltpu.VMEM((n, 3, pairs, 128), F32),
            dma((8,)),
            dma((2, PIECES)),
            dma((PIECES,)),
            dma((2, PIECES)),
            dma((BATCHES, PIECES)),
            dma((BATCHES, PIECES)),
            dma((BATCHES, PIECES)),
            dma((BATCHES, PIECES)),
            dma((n,)),
            dma((n,)),
            dma((n,)),
            dma((n,)),
        ],
        compiler_params=pltpu.CompilerParams(vmem_limit_bytes=VMEM_LIMIT, collective_id=0, has_side_effects=True),
        cost_estimate=pl.CostEstimate(flops=2 * n * own * depth * columns, bytes_accessed=1 << 27, transcendentals=0),
        name="gather_logits",
    )(x, w, lab)


PASSES = (((7,), ()), ((6, 5), (7,)), ((4, 3), (6, 5)), ((2, 1), (4, 3)), ((0,), (2, 1)), ((), (0,)))


def joins(k):
    return tuple(b for b in range(1, BATCHES) if BEFORE[b] == k)


def scatter_kernel(
    n, z_ref, w_ref, x_ref, top_ref, inv_ref, lab_ref,
    out_ref, g_ref, part_ref, give_ref, took_ref, pass_ref, came_ref, last_ref,
    z_v, g_v, top_s, inv_s, off_s, gw_v, z_sem, g_sem, gw_sem, pair_send, pair_recv, ici_send, ici_recv,
):
    me = lax.axis_index("tp")
    core = lax.rem(me, 2)
    half = z_ref.shape[1] // 2
    piece = half // PIECES
    depth, columns = w_ref.shape
    wide = 512

    groups = [[(k, 1) for k in given] + [(k, 0) for k in own] for given, own in PASSES]
    flat = [group for one in groups for group in one]

    def load(number):
        k, other = flat[number]
        return [
            pltpu.make_async_copy(
                z_ref.at[k, pl.ds(i * 2 * piece + other * piece, piece)],
                z_v.at[number % 2, pl.ds(i * piece, piece)],
                z_sem.at[number % 2, i],
            )
            for i in range(PIECES)
        ]

    def start(copies):
        for copy in copies:
            copy.start()
        return copies

    loading = start(load(0))
    meet(n, me)

    lane = lax.broadcasted_iota(jnp.int32, (32, 128), 1)
    sent = {}
    number = 0
    for given, own in PASSES:
        rows = half * (len(given) + len(own))
        g_copies = []
        for place, (k, other) in enumerate([(k, 1) for k in given] + [(k, 0) for k in own]):
            for i in range(PIECES):
                pair = lax.div(flip(me, 2 * MASKS[i][k]), 2) * PIECES + i
                for from_ref, to_ref in ((top_ref, top_s), (inv_ref, inv_s), (lab_ref, off_s)):
                    both = as_column(from_ref[pl.ds(pair, 1), :])
                    to_ref[pl.ds(i * piece, piece), :] = jnp.where(core == other, both[:piece], both[piece:])
            for copy in loading:
                copy.wait()
            slot = number % 2
            number += 1
            if number < len(flat):
                loading = start(load(number))

            def body(b, carry, slot=slot, place=place):
                part = pl.ds(pl.multiple_of(b * 32, 32), 32)
                to = pl.ds(pl.multiple_of(place * half + b * 32, 32), 32)
                top, inv, off = top_s[part, :], inv_s[part, :], off_s[part, :].astype(jnp.int32) - lane
                for c in range(0, columns, 128):
                    e = jnp.exp(z_v[slot, part, c : c + 128] - top) * inv
                    g_v[to, c : c + 128] = jnp.where(off == c, e - 1.0, e).astype(BF16)
                return carry

            lax.fori_loop(0, half // 32, body, 0)
            for i in range(PIECES):
                g_copies.append(
                    pltpu.make_async_copy(
                        g_v.at[pl.ds(place * half + i * piece, piece)],
                        g_ref.at[k, pl.ds(i * 2 * piece + other * piece, piece)],
                        g_sem.at[place, i],
                    )
                )
                g_copies[-1].start()

        arrivals = []
        for k in own:
            sent["pair", k].wait_recv()
            arrivals.append(took_ref.at[k])
            if k > 0:
                for b in joins(k):
                    for i in range(PIECES):
                        sent["ici", b, i].wait_recv()
                    arrivals.append(came_ref.at[b])
        results = [give_ref.at[k] for k in given] + [pass_ref.at[k] if k > 0 else last_ref for k in own]

        def multiply(*refs, given=given, own=own, rows=rows):
            w_tile, refs = refs[0], list(refs[1:])
            term = dot(g_v[:rows, :], w_tile[...], ((1,), (1,)))
            place = 0
            taken = len(own) + sum(len(joins(k)) for k in own if k > 0)
            ins, outs = refs[:taken], refs[taken:]
            for _ in given:
                outs.pop(0)[...] = term[place : place + half].astype(BF16)
                place += half
            for k in own:
                value = term[place : place + half]
                for _ in range(1 + (len(joins(k)) if k > 0 else 0)):
                    value = value + ins.pop(0)[...].astype(F32)
                out = outs.pop(0)
                out[...] = value.astype(out.dtype)
                place += half

        tile = pl.BlockSpec((half, wide), lambda j: (0, j))
        pltpu.emit_pipeline(
            multiply,
            grid=(depth // wide,),
            in_specs=[pl.BlockSpec((wide, columns), lambda j: (j, 0))] + [tile] * len(arrivals),
            out_specs=[tile] * len(results),
        )(w_ref, *arrivals, *results)
        for copy in g_copies:
            copy.wait()
        for k in own:
            if k > 0:
                for i in range(PIECES):
                    part = pl.ds(i * piece, piece)
                    sent["ici", k, i] = pltpu.make_async_remote_copy(
                        src_ref=pass_ref.at[k, part],
                        dst_ref=came_ref.at[k, part],
                        send_sem=ici_send.at[k, i],
                        recv_sem=ici_recv.at[k, i],
                        device_id=across(me, i, k),
                        device_id_type=MESH,
                    )
                    sent["ici", k, i].start()
        for k in given:
            sent["pair", k] = pltpu.make_async_remote_copy(
                src_ref=give_ref.at[k],
                dst_ref=took_ref.at[k],
                send_sem=pair_send.at[k],
                recv_sem=pair_recv.at[k],
                device_id={"tp": flip(me, 1)},
                device_id_type=MESH,
            )
            sent["pair", k].start()

    load_g = [
        pltpu.make_async_copy(g_ref.at[k], gw_v.at[pl.ds(k * 2 * half, 2 * half)], gw_sem.at[k]) for k in range(BATCHES)
    ]
    for copy in start(load_g):
        copy.wait()

    def outer(x_tile, out_tile):
        out_tile[...] = dot(x_tile[...], gw_v[...], ((0,), (0,))).astype(BF16)

    pltpu.emit_pipeline(
        outer,
        grid=(part_ref.shape[0] // BY_W_TALL,),
        in_specs=[pl.BlockSpec((BATCHES * 2 * half, BY_W_TALL), lambda j: (0, j))],
        out_specs=[pl.BlockSpec((BY_W_TALL, columns), lambda j: (j, 0))],
    )(x_ref, part_ref)

    for b in joins(0):
        for i in range(PIECES):
            sent["ici", b, i].wait_recv()

    def finish(last, *refs):
        value = last[...]
        for ref in refs[:-1]:
            value = value + ref[...].astype(F32)
        refs[-1][...] = value.astype(BF16)

    tile = pl.BlockSpec((half, 1024), lambda j: (0, j))
    pltpu.emit_pipeline(
        finish, grid=(depth // 1024,), in_specs=[tile] * (1 + len(joins(0))), out_specs=[tile]
    )(last_ref, *[came_ref.at[b] for b in joins(0)], out_ref)
    for copy in sent.values():
        copy.wait_send()


def scatter_call(n, z, w, xb, top, inv, lab):
    depth, columns = w.shape
    half = z.shape[1] // 2
    anywhere, vmem = pl.BlockSpec(memory_space=pl.ANY), pl.BlockSpec(memory_space=pltpu.VMEM)
    dma = pltpu.SemaphoreType.DMA
    moved = jax.ShapeDtypeStruct((BATCHES, half, depth), BF16)
    most = max(len(given) + len(own) for given, own in PASSES)
    return pl.pallas_call(
        functools.partial(scatter_kernel, n),
        in_specs=[anywhere, anywhere, anywhere, vmem, vmem, vmem],
        out_specs=[anywhere] * 8,
        out_shape=[
            jax.ShapeDtypeStruct((half, depth), BF16),
            jax.ShapeDtypeStruct(z.shape, BF16),
            jax.ShapeDtypeStruct((BY_W_EARLY * BY_W_TALL, columns), BF16),
            moved,
            moved,
            moved,
            moved,
            jax.ShapeDtypeStruct((half, depth), F32),
        ],
        scratch_shapes=[
            pltpu.VMEM((2, half, columns), F32),
            pltpu.VMEM((most * half, columns), BF16),
            pltpu.VMEM((half, 128), F32),
            pltpu.VMEM((half, 128), F32),
            pltpu.VMEM((half, 128), F32),
            pltpu.VMEM((BATCHES * 2 * half, columns), BF16),
            dma((2, PIECES)),
            dma((most, PIECES)),
            dma((BATCHES,)),
            dma((BATCHES,)),
            dma((BATCHES,)),
            dma((BATCHES, PIECES)),
            dma((BATCHES, PIECES)),
        ],
        compiler_params=pltpu.CompilerParams(vmem_limit_bytes=VMEM_LIMIT, collective_id=1, has_side_effects=True),
        cost_estimate=pl.CostEstimate(flops=3 * n * half * depth * columns, bytes_accessed=1 << 28, transcendentals=0),
        name="by_x_scatter",
    )(z, w, xb, top, inv, lab)


def by_w_kernel(x_ref, g_ref, part_ref, out_ref, g_v, part_v, g_sem, part_sem):
    rows, columns = g_ref.shape
    early = part_ref.shape[0]
    g_load = [
        pltpu.make_async_copy(g_ref.at[pl.ds(p * rows // 8, rows // 8)], g_v.at[pl.ds(p * rows // 8, rows // 8)], g_sem.at[p])
        for p in range(8)
    ]
    load = pltpu.make_async_copy(part_ref, part_v, part_sem.at[0])
    for copy in g_load:
        copy.start()
    load.start()
    for copy in g_load:
        copy.wait()

    def outer(x_tile, out_tile):
        out_tile[...] = dot(x_tile[...], g_v[...], ((0,), (0,))).astype(BF16)

    tiles = (out_ref.shape[0] - early) // BY_W_TALL

    def run(first, count):
        skip = early // BY_W_TALL + first
        pltpu.emit_pipeline(
            outer,
            grid=(count,),
            in_specs=[pl.BlockSpec((rows, BY_W_TALL), lambda j: (0, skip + j))],
            out_specs=[pl.BlockSpec((BY_W_TALL, columns), lambda j: (skip + j, 0))],
        )(x_ref, out_ref)

    run(0, tiles // 2)
    load.wait()
    store = pltpu.make_async_copy(part_v, out_ref.at[pl.ds(0, early)], part_sem.at[1])
    store.start()
    run(tiles // 2, tiles - tiles // 2)
    store.wait()


def by_w_call(xb, g, part):
    rows, depth = xb.shape
    columns = g.shape[1]
    anywhere = pl.BlockSpec(memory_space=pl.ANY)
    dma = pltpu.SemaphoreType.DMA
    return pl.pallas_call(
        by_w_kernel,
        in_specs=[anywhere] * 3,
        out_specs=anywhere,
        out_shape=jax.ShapeDtypeStruct((depth, columns), BF16),
        scratch_shapes=[pltpu.VMEM((rows, columns), BF16), pltpu.VMEM(part.shape, BF16), dma((8,)), dma((2,))],
        compiler_params=pltpu.CompilerParams(vmem_limit_bytes=VMEM_LIMIT),
        cost_estimate=pl.CostEstimate(flops=rows * depth * columns, bytes_accessed=1 << 26, transcendentals=0),
        name="by_w",
    )(xb, g, part)


def solution(mesh):
    n = mesh.shape["tp"]

    def step(x, w, label):
        me, own, columns = lax.axis_index("tp"), x.shape[0], w.shape[1]
        piece = own // PIECES
        lab = jnp.pad(label.reshape(PIECES, piece), ((0, 0), (0, 128 - piece)))
        xb, z, labs, top, inv, loss = logits_call(n, x, w, lab)
        mine = labs[:, :, :piece].reshape(n // 2, 2, PIECES, piece).swapaxes(1, 2).reshape(-1, 128) - me * columns
        by_x, g, part, *_ = scatter_call(n, z, w, xb.reshape(-1, xb.shape[-1]), top, inv, mine.astype(F32))
        by_w = by_w_call(xb.reshape(-1, xb.shape[-1]), g.reshape(-1, columns), part)
        by_device = loss.reshape(n // 2, PIECES, 2, piece).swapaxes(1, 2).reshape(n, own)
        return lax.dynamic_index_in_dim(by_device, me, 0, keepdims=False), by_x, by_w

    return jax.shard_map(
        step,
        mesh=mesh,
        in_specs=(P(("dp", "tp"), None), P(None, "tp"), P(("dp", "tp"))),
        out_specs=(P(("dp", "tp")), P(("dp", "tp"), None), P("dp", "tp")),
        check_vma=False,
    )
```

```python
import functools

import jax
import jax.numpy as jnp
from jax import lax
from jax.experimental import pallas as pl
from jax.experimental.pallas import tpu as pltpu
from jax.sharding import PartitionSpec as P

F32, BF16 = jnp.float32, jnp.bfloat16
MESH = pl.DeviceIdType.MESH
VMEM_LIMIT = 63 * 1024 * 1024

ORDERS = ((4, 2, 1), (2, 1, 4), (1, 4, 2))
MASKS = tuple((0, a, b, c, a | b, a | c, b | c, a | b | c) for a, b, c in ORDERS)
LAST = (None, 0, 1, 2, 1, 2, 2, 2)
BEFORE = (None, 0, 0, 0, 1, 1, 2, 4)
BATCHES, PIECES = 8, 3
BY_W_TALL = 256
BY_W_EARLY = 10


def dot(a, b, contract):
    return lax.dot_general(a, b, (contract, ((), ())), preferred_element_type=F32)


def flip(index, mask):
    for bit in (1, 2, 4, 8):
        if mask & bit:
            index = index + bit - 2 * bit * lax.rem(lax.div(index, bit), 2)
    return index


def across(me, i, k):
    return {"tp": flip(me, 2 * ORDERS[i][LAST[k]])}


def meet(n, me):
    barrier = pltpu.get_barrier_semaphore()
    for j in range(1, n):
        pl.semaphore_signal(barrier, inc=1, device_id={"tp": lax.rem(me + j, n)}, device_id_type=MESH)
    pl.semaphore_wait(barrier, n - 1)


def to_all(n, me, own_ref, all_ref, send_sems, recv_sems):
    copies = []
    for j in range(1, n):
        copies.append(
            pltpu.make_async_remote_copy(
                src_ref=own_ref,
                dst_ref=all_ref.at[me],
                send_sem=send_sems.at[j],
                recv_sem=recv_sems.at[j],
                device_id={"tp": lax.rem(me + j, n)},
                device_id_type=MESH,
            )
        )
    for copy in copies:
        copy.start()
    return copies


def as_column(row):
    return jnp.broadcast_to(row, (128, 128)).T


def logits_kernel(
    n, x_ref, w_ref, lab_ref, xb_ref, z_ref, labs_ref, top_ref, inv_ref, loss_ref,
    w_v, x_v, z_v, m_s, s_s, r_s, off_s, st_s, own_s, all_s,
    w_sem, x_sem, keep_sem, z_sem, ici_send, ici_recv, pair_send, pair_recv, lab_send, lab_recv, st_send, st_recv,
):
    me = lax.axis_index("tp")
    core = lax.rem(me, 2)
    piece = x_ref.shape[0] // PIECES
    half = PIECES * piece
    depth, columns = w_ref.shape
    wide = 256

    w_parts = 8
    w_copies = []
    for p in range(w_parts):
        part = pl.ds(p * (depth // w_parts), depth // w_parts)
        w_copies.append(pltpu.make_async_copy(w_ref.at[part], w_v.at[part], w_sem.at[p]))
        w_copies[-1].start()
    x_load = pltpu.make_async_copy(x_ref, x_v.at[0], x_sem.at[0, 0])
    x_load.start()

    meet(n, me)

    def slot(k, i, other):
        return xb_ref.at[k, pl.ds(i * 2 * piece + other * piece, piece)]

    def source(k, i):
        return x_ref.at[pl.ds(i * piece, piece)] if k == 0 else slot(k, i, 0)

    sent = {}

    def send(k, i):
        sent["ici", k, i] = pltpu.make_async_remote_copy(
            src_ref=source(BEFORE[k], i),
            dst_ref=slot(k, i, 0),
            send_sem=ici_send.at[k, i],
            recv_sem=ici_recv.at[k, i],
            device_id=across(me, i, k),
            device_id_type=MESH,
        )
        sent["ici", k, i].start()

    def share(k, i):
        sent["pair", k, i] = pltpu.make_async_remote_copy(
            src_ref=source(k, i),
            dst_ref=slot(k, i, 1),
            send_sem=pair_send.at[k, i],
            recv_sem=pair_recv.at[k, i],
            device_id={"tp": flip(me, 1)},
            device_id_type=MESH,
        )
        sent["pair", k, i].start()

    labels = to_all(n, me, lab_ref, labs_ref, lab_send, lab_recv)
    for i in range(PIECES):
        send(1, i)
    for i in range(PIECES):
        share(0, i)
    for k in (2, 3):
        for i in range(PIECES):
            send(k, i)
    labs_ref[me] = lab_ref[...]
    x_load.wait()
    kept = []
    for i in range(PIECES):
        kept.append(pltpu.make_async_copy(x_v.at[0, pl.ds(i * piece, piece)], slot(0, i, 0), keep_sem.at[i]))
        kept[-1].start()
    for copy in labels:
        copy.wait_recv()

    z_copies = {0: [], 1: []}
    lane = lax.broadcasted_iota(jnp.int32, (half, 128), 1)

    def compute(k, other):
        for i in range(PIECES):
            dev = flip(me, 2 * MASKS[i][k] + other)
            row = (labs_ref[dev, pl.ds(i, 1), :] - me * columns).astype(F32)
            off_s[pl.ds(i * piece, piece), :] = as_column(row)[:piece].astype(jnp.int32)
        m_s[...] = jnp.full(m_s.shape, -jnp.inf, F32)
        s_s[...] = jnp.zeros(s_s.shape, F32)
        r_s[...] = jnp.zeros(r_s.shape, F32)
        for copy in z_copies[other]:
            copy.wait()

        def body(j, carry):
            at = pl.multiple_of(j * wide, wide)
            z = dot(x_v[other], w_v[:, pl.ds(at, wide)], ((1,), (0,)))
            z_v[other, :, pl.ds(at, wide)] = z
            old = m_s[...]
            new = old
            for c in range(0, wide, 128):
                new = jnp.maximum(new, z[:, c : c + 128])
            total = s_s[...] * jnp.exp(old - new)
            right = r_s[...]
            off = off_s[...] - at
            for c in range(0, wide, 128):
                total += jnp.exp(z[:, c : c + 128] - new)
                right += jnp.where(lane == off - c, z[:, c : c + 128], 0.0)
            m_s[...] = new
            s_s[...] = total
            r_s[...] = right
            return carry

        lax.fori_loop(0, columns // wide, body, 0)
        z_copies[other] = []
        for i in range(PIECES):
            z_copies[other].append(
                pltpu.make_async_copy(
                    z_v.at[other, pl.ds(i * piece, piece)],
                    z_ref.at[k, pl.ds(i * 2 * piece + other * piece, piece)],
                    z_sem.at[other, i],
                )
            )
            z_copies[other][-1].start()
        high = jnp.max(m_s[...], -1, keepdims=True)
        total = jnp.sum(s_s[...] * jnp.exp(m_s[...] - high), -1, keepdims=True)
        right = jnp.sum(r_s[...], -1, keepdims=True)
        st_s[other] = jnp.where(lane == 0, high, jnp.where(lane == 1, total, jnp.where(lane == 2, right, 0.0)))

    def load(k, other):
        copies = []
        for i in range(PIECES):
            copies.append(pltpu.make_async_copy(slot(k, i, other), x_v.at[other, pl.ds(i * piece, piece)], x_sem.at[other, i]))
            copies[-1].start()
        return copies

    def wait(copies):
        for copy in copies:
            copy.wait()

    def load_shared(k):
        for i in range(PIECES):
            sent["pair", k, i].wait_recv()
        return load(k, 1)

    def arrive(k):
        for i in range(PIECES):
            sent["ici", k, i].wait_recv()
        for i in range(PIECES):
            for later in range(4, BATCHES):
                if BEFORE[later] == k:
                    send(later, i)
        for i in range(PIECES):
            share(k, i)
        return load(k, 0)

    last = BATCHES - 1
    own_load, shared_load = [], load_shared(0)
    wait(w_copies)
    for k in range(BATCHES):
        compute(k, 0)
        if k == 0:
            wait(kept)
        if k + 1 < last:
            own_load = arrive(k + 1)
        if k == last:
            shared_load = load_shared(k)
        wait(shared_load)
        compute(k, 1)
        if k + 1 == last:
            own_load = arrive(last)
        elif k < last:
            shared_load = load_shared(k + 1)
        for i in range(PIECES):
            part = pl.ds(i * piece, piece)
            first, second = st_s[0, part, :], st_s[1, part, :]
            both = jnp.concatenate(
                [jnp.where(core == 0, first, second), jnp.where(core == 0, second, first)], 0
            ).T
            pair = lax.div(flip(me, 2 * MASKS[i][k]), 2) * PIECES + i
            for t in range(3):
                own_s[t, pl.ds(pair, 1), :] = both[t : t + 1, :]
        if k < last:
            wait(own_load)

    stats = to_all(n, me, own_s, all_s, st_send, st_recv)
    all_s[me] = own_s[...]
    for copy in stats:
        copy.wait_recv()
    high, sums, right = all_s[:, 0], all_s[:, 1], all_s[:, 2]
    top = jnp.max(high, 0)
    total = jnp.sum(sums * jnp.exp(high - top[None]), 0)
    top_ref[...] = top
    inv_ref[...] = 1.0 / total
    loss_ref[...] = jnp.log(total) + top - jnp.sum(right, 0)
    for copy in labels + stats + list(sent.values()):
        copy.wait_send()
    for copies in z_copies.values():
        for copy in copies:
            copy.wait()


def logits_call(n, x, w, lab):
    own, depth = x.shape
    columns = w.shape[1]
    pairs = n // 2 * PIECES
    anywhere, vmem = pl.BlockSpec(memory_space=pl.ANY), pl.BlockSpec(memory_space=pltpu.VMEM)
    dma = pltpu.SemaphoreType.DMA
    return pl.pallas_call(
        functools.partial(logits_kernel, n),
        in_specs=[anywhere, anywhere, vmem],
        out_specs=[anywhere, anywhere, vmem, vmem, vmem, vmem],
        out_shape=[
            jax.ShapeDtypeStruct((BATCHES, 2 * own, depth), BF16),
            jax.ShapeDtypeStruct((BATCHES, 2 * own, columns), F32),
            jax.ShapeDtypeStruct((n,) + lab.shape, jnp.int32),
            jax.ShapeDtypeStruct((pairs, 128), F32),
            jax.ShapeDtypeStruct((pairs, 128), F32),
            jax.ShapeDtypeStruct((pairs, 128), F32),
        ],
        scratch_shapes=[
            pltpu.VMEM((depth, columns), BF16),
            pltpu.VMEM((2, own, depth), BF16),
            pltpu.VMEM((2, own, columns), F32),
            pltpu.VMEM((own, 128), F32),
            pltpu.VMEM((own, 128), F32),
            pltpu.VMEM((own, 128), F32),
            pltpu.VMEM((own, 128), jnp.int32),
            pltpu.VMEM((2, own, 128), F32),
            pltpu.VMEM((3, pairs, 128), F32),
            pltpu.VMEM((n, 3, pairs, 128), F32),
            dma((8,)),
            dma((2, PIECES)),
            dma((PIECES,)),
            dma((2, PIECES)),
            dma((BATCHES, PIECES)),
            dma((BATCHES, PIECES)),
            dma((BATCHES, PIECES)),
            dma((BATCHES, PIECES)),
            dma((n,)),
            dma((n,)),
            dma((n,)),
            dma((n,)),
        ],
        compiler_params=pltpu.CompilerParams(vmem_limit_bytes=VMEM_LIMIT, collective_id=0, has_side_effects=True),
        cost_estimate=pl.CostEstimate(flops=2 * n * own * depth * columns, bytes_accessed=1 << 27, transcendentals=0),
        name="gather_logits",
    )(x, w, lab)


PASSES = tuple((7 - t if t < 8 else None, 8 - t if t > 0 else None) for t in range(9))


def joins(k):
    return tuple(b for b in range(1, BATCHES) if BEFORE[b] == k)


def scatter_kernel(
    n, z_ref, w_ref, x_ref, top_ref, inv_ref, lab_ref,
    out_ref, g_ref, part_ref, took_ref, pass_ref, came_ref,
    z_v, g_v, w_v, in_v, p_v, o_v, last_v, fin_v, top_s, inv_s, off_s, gw_v,
    z_sem, g_sem, w_sem, in_sem, p_sem, o_sem, fin_sem, gw_sem, pair_recv, ici_send, ici_recv,
):
    me = lax.axis_index("tp")
    core = lax.rem(me, 2)
    half = z_ref.shape[1] // 2
    piece = half // PIECES
    depth, columns = w_ref.shape
    wide = w_v.shape[1]
    steps = depth // wide

    groups = [[(k, other) for k, other in ((given, 1), (own, 0)) if k is not None] for given, own in PASSES]
    flat = [group for one in groups for group in one]

    def start(copies):
        for copy in copies:
            copy.start()
        return copies

    def wait(copies):
        for copy in copies:
            copy.wait()

    def load_z(number):
        k, other = flat[number]
        return [
            pltpu.make_async_copy(
                z_ref.at[k, pl.ds(i * 2 * piece + other * piece, piece)],
                z_v.at[number % 2, pl.ds(i * piece, piece)],
                z_sem.at[number % 2, i],
            )
            for i in range(PIECES)
        ]

    def columns_at(j):
        return pl.ds(pl.multiple_of(j * wide, wide), wide)

    def load_w(j, slot):
        return pltpu.make_async_copy(w_ref.at[columns_at(j)], w_v.at[slot], w_sem.at[slot])

    loading = start(load_z(0))
    load_w(0, 0).start()
    meet(n, me)

    lane = lax.broadcasted_iota(jnp.int32, (32, 128), 1)
    sent, load_g = {}, []
    number = 0
    for t, (given, own) in enumerate(PASSES):
        places = {group: place for place, group in enumerate(groups[t])}
        rows = half * len(places)
        g_copies = []
        for (k, other), place in places.items():
            for i in range(PIECES):
                pair = lax.div(flip(me, 2 * MASKS[i][k]), 2) * PIECES + i
                for from_ref, to_ref in ((top_ref, top_s), (inv_ref, inv_s), (lab_ref, off_s)):
                    both = as_column(from_ref[pl.ds(pair, 1), :])
                    to_ref[pl.ds(i * piece, piece), :] = jnp.where(core == other, both[:piece], both[piece:])
            wait(loading)
            slot = number % 2
            number += 1
            if number < len(flat):
                loading = start(load_z(number))

            def body(b, carry, slot=slot, place=place):
                part = pl.ds(pl.multiple_of(b * 32, 32), 32)
                to = pl.ds(pl.multiple_of(place * half + b * 32, 32), 32)
                top, inv, off = top_s[part, :], inv_s[part, :], off_s[part, :].astype(jnp.int32) - lane
                for c in range(0, columns, 128):
                    e = jnp.exp(z_v[slot, part, c : c + 128] - top) * inv
                    g_v[to, c : c + 128] = jnp.where(off == c, e - 1.0, e).astype(BF16)
                return carry

            lax.fori_loop(0, half // 32, body, 0)
            for i in range(PIECES):
                g_copies.append(
                    pltpu.make_async_copy(
                        g_v.at[pl.ds(place * half + i * piece, piece)],
                        g_ref.at[k, pl.ds(i * 2 * piece + other * piece, piece)],
                        g_sem.at[place, i],
                    )
                )
                g_copies[-1].start()

        arrivals = []
        if own is not None:
            pltpu.make_async_remote_copy(
                src_ref=took_ref.at[own],
                dst_ref=took_ref.at[own],
                send_sem=p_sem.at[0],
                recv_sem=pair_recv.at[own],
                device_id={"tp": flip(me, 1)},
                device_id_type=MESH,
            ).wait_recv()
            arrivals.append(took_ref.at[own])
            for b in joins(own) if own else ():
                for i in range(PIECES):
                    sent[b, i].wait_recv()
                arrivals.append(came_ref.at[b])

        def load_in(j, slot, arrivals=arrivals):
            return [
                pltpu.make_async_copy(ref.at[:, columns_at(j)], in_v.at[slot, m], in_sem.at[slot, m])
                for m, ref in enumerate(arrivals)
            ]

        def outs(j, slot, given=given, own=own):
            copies = []
            if given is not None:
                copies.append(
                    pltpu.make_async_remote_copy(
                        src_ref=p_v.at[slot],
                        dst_ref=took_ref.at[given, :, columns_at(j)],
                        send_sem=p_sem.at[slot],
                        recv_sem=pair_recv.at[given],
                        device_id={"tp": flip(me, 1)},
                        device_id_type=MESH,
                    )
                )
            if own:
                copies.append(pltpu.make_async_copy(o_v.at[slot], pass_ref.at[own, :, columns_at(j)], o_sem.at[slot]))
            return copies

        def finished(copies, given=given):
            for m, copy in enumerate(copies):
                if m == 0 and given is not None:
                    copy.wait_send()
                else:
                    copy.wait()

        start(load_in(0, 0))

        def multiply(j, carry, t=t, given=given, own=own, rows=rows, load_in=load_in, outs=outs, finished=finished, count=len(arrivals)):
            slot = lax.rem(j, 2)
            if t < len(PASSES) - 1:
                load_w(lax.rem(j + 1, steps), 1 - slot).start()

            @pl.when(j + 1 < steps)
            def _():
                if t == len(PASSES) - 1:
                    load_w(j + 1, 1 - slot).start()
                start(load_in(j + 1, 1 - slot))

            @pl.when(j > 0)
            def _():
                start(outs(j - 1, 1 - slot))

            @pl.when(j > 1)
            def _():
                finished(outs(j - 2, slot))

            load_w(j, slot).wait()
            wait(load_in(j, slot))
            term = dot(g_v[:rows, :], w_v[slot], ((1,), (1,)))
            if given is not None:
                p_v[slot] = term[:half].astype(BF16)
            if own is not None:
                value = term[rows - half :]
                for m in range(count):
                    value = value + in_v[slot, m].astype(F32)
                if own:
                    o_v[slot] = value.astype(BF16)
                else:
                    last_v[:, columns_at(j)] = value
            return carry

        lax.fori_loop(0, steps, multiply, 0)
        start(outs(steps - 1, (steps - 1) % 2))
        for j in (steps - 2, steps - 1):
            finished(outs(j, j % 2))
        wait(g_copies)
        if own is not None:
            for i in range(PIECES if own else 0):
                part = pl.ds(i * piece, piece)
                sent[own, i] = pltpu.make_async_remote_copy(
                    src_ref=pass_ref.at[own, part],
                    dst_ref=came_ref.at[own, part],
                    send_sem=ici_send.at[own, i],
                    recv_sem=ici_recv.at[own, i],
                    device_id=across(me, i, own),
                    device_id_type=MESH,
                )
                sent[own, i].start()
            load_g += start([pltpu.make_async_copy(g_ref.at[own], gw_v.at[pl.ds(own * 2 * half, 2 * half)], gw_sem.at[own])])

    wait(load_g)

    def outer(x_tile, out_tile):
        out_tile[...] = dot(x_tile[...], gw_v[...], ((0,), (0,))).astype(BF16)

    pltpu.emit_pipeline(
        outer,
        grid=(part_ref.shape[0] // BY_W_TALL,),
        in_specs=[pl.BlockSpec((BATCHES * 2 * half, BY_W_TALL), lambda j: (0, j))],
        out_specs=[pl.BlockSpec((BY_W_TALL, columns), lambda j: (j, 0))],
    )(x_ref, part_ref)

    ends = []
    for m, b in enumerate(reversed(joins(0))):
        for i in range(PIECES):
            sent[b, i].wait_recv()
        ends += start([pltpu.make_async_copy(came_ref.at[b], fin_v.at[m], fin_sem.at[m])])
    wait(ends)

    def finish(j, carry):
        at = columns_at(j)
        value = last_v[:, at]
        for m in range(len(joins(0))):
            value = value + fin_v[m, :, at].astype(F32)
        fin_v[0, :, at] = value.astype(BF16)
        return carry

    lax.fori_loop(0, steps, finish, 0)
    wait(start([pltpu.make_async_copy(fin_v.at[0], out_ref, fin_sem.at[0])]))
    for copy in sent.values():
        copy.wait_send()


def scatter_call(n, z, w, xb, top, inv, lab):
    depth, columns = w.shape
    half, wide = z.shape[1] // 2, 512
    anywhere, vmem = pl.BlockSpec(memory_space=pl.ANY), pl.BlockSpec(memory_space=pltpu.VMEM)
    dma = pltpu.SemaphoreType.DMA
    moved = jax.ShapeDtypeStruct((BATCHES, half, depth), BF16)
    most = 1 + max(len(joins(k)) for k in range(1, BATCHES))
    return pl.pallas_call(
        functools.partial(scatter_kernel, n),
        in_specs=[anywhere, anywhere, anywhere, vmem, vmem, vmem],
        out_specs=[anywhere] * 6,
        out_shape=[
            jax.ShapeDtypeStruct((half, depth), BF16),
            jax.ShapeDtypeStruct(z.shape, BF16),
            jax.ShapeDtypeStruct((BY_W_EARLY * BY_W_TALL, columns), BF16),
            moved,
            moved,
            moved,
        ],
        scratch_shapes=[
            pltpu.VMEM((2, half, columns), F32),
            pltpu.VMEM((2 * half, columns), BF16),
            pltpu.VMEM((2, wide, columns), BF16),
            pltpu.VMEM((2, most, half, wide), BF16),
            pltpu.VMEM((2, half, wide), BF16),
            pltpu.VMEM((2, half, wide), BF16),
            pltpu.VMEM((half, depth), F32),
            pltpu.VMEM((len(joins(0)), half, depth), BF16),
            pltpu.VMEM((half, 128), F32),
            pltpu.VMEM((half, 128), F32),
            pltpu.VMEM((half, 128), F32),
            pltpu.VMEM((BATCHES * 2 * half, columns), BF16),
            dma((2, PIECES)),
            dma((2, PIECES)),
            dma((2,)),
            dma((2, most)),
            dma((2,)),
            dma((2,)),
            dma((3,)),
            dma((BATCHES,)),
            dma((BATCHES,)),
            dma((BATCHES, PIECES)),
            dma((BATCHES, PIECES)),
        ],
        compiler_params=pltpu.CompilerParams(vmem_limit_bytes=VMEM_LIMIT, collective_id=1, has_side_effects=True),
        cost_estimate=pl.CostEstimate(flops=3 * n * half * depth * columns, bytes_accessed=1 << 28, transcendentals=0),
        name="by_x_scatter",
    )(z, w, xb, top, inv, lab)


def by_w_kernel(x_ref, g_ref, part_ref, out_ref, g_v, part_v, g_sem, part_sem):
    rows, columns = g_ref.shape
    early = part_ref.shape[0]
    g_load = [
        pltpu.make_async_copy(g_ref.at[pl.ds(p * rows // 8, rows // 8)], g_v.at[pl.ds(p * rows // 8, rows // 8)], g_sem.at[p])
        for p in range(8)
    ]
    load = pltpu.make_async_copy(part_ref, part_v, part_sem.at[0])
    for copy in g_load:
        copy.start()
    load.start()
    for copy in g_load:
        copy.wait()

    def outer(x_tile, out_tile):
        out_tile[...] = dot(x_tile[...], g_v[...], ((0,), (0,))).astype(BF16)

    tiles = (out_ref.shape[0] - early) // BY_W_TALL

    def run(first, count):
        skip = early // BY_W_TALL + first
        pltpu.emit_pipeline(
            outer,
            grid=(count,),
            in_specs=[pl.BlockSpec((rows, BY_W_TALL), lambda j: (0, skip + j))],
            out_specs=[pl.BlockSpec((BY_W_TALL, columns), lambda j: (skip + j, 0))],
        )(x_ref, out_ref)

    run(0, tiles // 2)
    load.wait()
    store = pltpu.make_async_copy(part_v, out_ref.at[pl.ds(0, early)], part_sem.at[1])
    store.start()
    run(tiles // 2, tiles - tiles // 2)
    store.wait()


def by_w_call(xb, g, part):
    rows, depth = xb.shape
    columns = g.shape[1]
    anywhere = pl.BlockSpec(memory_space=pl.ANY)
    dma = pltpu.SemaphoreType.DMA
    return pl.pallas_call(
        by_w_kernel,
        in_specs=[anywhere] * 3,
        out_specs=anywhere,
        out_shape=jax.ShapeDtypeStruct((depth, columns), BF16),
        scratch_shapes=[pltpu.VMEM((rows, columns), BF16), pltpu.VMEM(part.shape, BF16), dma((8,)), dma((2,))],
        compiler_params=pltpu.CompilerParams(vmem_limit_bytes=VMEM_LIMIT),
        cost_estimate=pl.CostEstimate(flops=rows * depth * columns, bytes_accessed=1 << 26, transcendentals=0),
        name="by_w",
    )(xb, g, part)


def solution(mesh):
    n = mesh.shape["tp"]

    def step(x, w, label):
        me, own, columns = lax.axis_index("tp"), x.shape[0], w.shape[1]
        piece = own // PIECES
        lab = jnp.pad(label.reshape(PIECES, piece), ((0, 0), (0, 128 - piece)))
        xb, z, labs, top, inv, loss = logits_call(n, x, w, lab)
        mine = labs[:, :, :piece].reshape(n // 2, 2, PIECES, piece).swapaxes(1, 2).reshape(-1, 128) - me * columns
        by_x, g, part, *_ = scatter_call(n, z, w, xb.reshape(-1, xb.shape[-1]), top, inv, mine.astype(F32))
        by_w = by_w_call(xb.reshape(-1, xb.shape[-1]), g.reshape(-1, columns), part)
        by_device = loss.reshape(n // 2, PIECES, 2, piece).swapaxes(1, 2).reshape(n, own)
        return lax.dynamic_index_in_dim(by_device, me, 0, keepdims=False), by_x, by_w

    return jax.shard_map(
        step,
        mesh=mesh,
        in_specs=(P(("dp", "tp"), None), P(None, "tp"), P(("dp", "tp"))),
        out_specs=(P(("dp", "tp")), P(("dp", "tp"), None), P("dp", "tp")),
        check_vma=False,
    )
```

```python
import functools

import jax
import jax.numpy as jnp
from jax import lax
from jax.experimental import pallas as pl
from jax.experimental.pallas import tpu as pltpu
from jax.sharding import PartitionSpec as P

F32, BF16 = jnp.float32, jnp.bfloat16
MESH = pl.DeviceIdType.MESH
VMEM_LIMIT = 63 * 1024 * 1024

ORDERS = ((4, 2, 1), (2, 1, 4), (1, 4, 2))
MASKS = tuple((0, a, b, c, a | b, a | c, b | c, a | b | c) for a, b, c in ORDERS)
LAST = (None, 0, 1, 2, 1, 2, 2, 2)
BEFORE = (None, 0, 0, 0, 1, 1, 2, 4)
BATCHES, PIECES = 8, 3
BY_W_TALL = 512
BY_W_EARLY = 5


def dot(a, b, contract):
    return lax.dot_general(a, b, (contract, ((), ())), preferred_element_type=F32)


def flip(index, mask):
    for bit in (1, 2, 4, 8):
        if mask & bit:
            index = index + bit - 2 * bit * lax.rem(lax.div(index, bit), 2)
    return index


def across(me, i, k):
    return {"tp": flip(me, 2 * ORDERS[i][LAST[k]])}


def meet(n, me):
    barrier = pltpu.get_barrier_semaphore()
    for j in range(1, n):
        pl.semaphore_signal(barrier, inc=1, device_id={"tp": lax.rem(me + j, n)}, device_id_type=MESH)
    pl.semaphore_wait(barrier, n - 1)


def to_all(n, me, own_ref, all_ref, send_sems, recv_sems):
    copies = []
    for j in range(1, n):
        copies.append(
            pltpu.make_async_remote_copy(
                src_ref=own_ref,
                dst_ref=all_ref.at[me],
                send_sem=send_sems.at[j],
                recv_sem=recv_sems.at[j],
                device_id={"tp": lax.rem(me + j, n)},
                device_id_type=MESH,
            )
        )
    for copy in copies:
        copy.start()
    return copies


def as_column(row):
    return jnp.broadcast_to(row, (128, 128)).T


def logits_kernel(
    n, x_ref, w_ref, lab_ref, xb_ref, z_ref, labs_ref, top_ref, inv_ref, loss_ref,
    w_v, x_v, z_v, m_s, s_s, r_s, off_s, st_s, own_s, all_s,
    w_sem, x_sem, keep_sem, z_sem, ici_send, ici_recv, pair_send, pair_recv, lab_send, lab_recv, st_send, st_recv,
):
    me = lax.axis_index("tp")
    core = lax.rem(me, 2)
    piece = x_ref.shape[0] // PIECES
    half = PIECES * piece
    depth, columns = w_ref.shape
    wide = 512

    w_parts = 8
    w_copies = []
    for p in range(w_parts):
        part = pl.ds(p * (depth // w_parts), depth // w_parts)
        w_copies.append(pltpu.make_async_copy(w_ref.at[part], w_v.at[part], w_sem.at[p]))
        w_copies[-1].start()
    x_load = pltpu.make_async_copy(x_ref, x_v.at[0], x_sem.at[0, 0])
    x_load.start()

    meet(n, me)

    def slot(k, i, other):
        return xb_ref.at[k, pl.ds(i * 2 * piece + other * piece, piece)]

    def source(k, i):
        return x_ref.at[pl.ds(i * piece, piece)] if k == 0 else slot(k, i, 0)

    sent = {}

    def send(k, i):
        sent["ici", k, i] = pltpu.make_async_remote_copy(
            src_ref=source(BEFORE[k], i),
            dst_ref=slot(k, i, 0),
            send_sem=ici_send.at[k, i],
            recv_sem=ici_recv.at[k, i],
            device_id=across(me, i, k),
            device_id_type=MESH,
        )
        sent["ici", k, i].start()

    def share(k, i):
        sent["pair", k, i] = pltpu.make_async_remote_copy(
            src_ref=source(k, i),
            dst_ref=slot(k, i, 1),
            send_sem=pair_send.at[k, i],
            recv_sem=pair_recv.at[k, i],
            device_id={"tp": flip(me, 1)},
            device_id_type=MESH,
        )
        sent["pair", k, i].start()

    labels = to_all(n, me, lab_ref, labs_ref, lab_send, lab_recv)
    for i in range(PIECES):
        send(1, i)
    for i in range(PIECES):
        share(0, i)
    for k in (2, 3):
        for i in range(PIECES):
            send(k, i)
    labs_ref[me] = lab_ref[...]
    x_load.wait()
    kept = []
    for i in range(PIECES):
        kept.append(pltpu.make_async_copy(x_v.at[0, pl.ds(i * piece, piece)], slot(0, i, 0), keep_sem.at[i]))
        kept[-1].start()
    for copy in labels:
        copy.wait_recv()

    z_copies = {0: [], 1: []}
    lane = lax.broadcasted_iota(jnp.int32, (half, 128), 1)

    def compute(k, other):
        for i in range(PIECES):
            dev = flip(me, 2 * MASKS[i][k] + other)
            row = (labs_ref[dev, pl.ds(i, 1), :] - me * columns).astype(F32)
            off_s[pl.ds(i * piece, piece), :] = as_column(row)[:piece].astype(jnp.int32)
        m_s[...] = jnp.full(m_s.shape, -jnp.inf, F32)
        s_s[...] = jnp.zeros(s_s.shape, F32)
        r_s[...] = jnp.zeros(r_s.shape, F32)
        for copy in z_copies[other]:
            copy.wait()

        def body(j, carry):
            at = pl.multiple_of(j * wide, wide)
            z = dot(x_v[other], w_v[:, pl.ds(at, wide)], ((1,), (0,)))
            z_v[other, :, pl.ds(at, wide)] = z
            old = m_s[...]
            new = old
            for c in range(0, wide, 128):
                new = jnp.maximum(new, z[:, c : c + 128])
            total = s_s[...] * jnp.exp(old - new)
            right = r_s[...]
            off = off_s[...] - at
            for c in range(0, wide, 128):
                total += jnp.exp(z[:, c : c + 128] - new)
                right += jnp.where(lane == off - c, z[:, c : c + 128], 0.0)
            m_s[...] = new
            s_s[...] = total
            r_s[...] = right
            return carry

        lax.fori_loop(0, columns // wide, body, 0)
        z_copies[other] = []
        for i in range(PIECES):
            z_copies[other].append(
                pltpu.make_async_copy(
                    z_v.at[other, pl.ds(i * piece, piece)],
                    z_ref.at[k, pl.ds(i * 2 * piece + other * piece, piece)],
                    z_sem.at[other, i],
                )
            )
            z_copies[other][-1].start()
        high = jnp.max(m_s[...], -1, keepdims=True)
        total = jnp.sum(s_s[...] * jnp.exp(m_s[...] - high), -1, keepdims=True)
        right = jnp.sum(r_s[...], -1, keepdims=True)
        st_s[other] = jnp.where(lane == 0, high, jnp.where(lane == 1, total, jnp.where(lane == 2, right, 0.0)))

    def load(k, other):
        copies = []
        for i in range(PIECES):
            copies.append(pltpu.make_async_copy(slot(k, i, other), x_v.at[other, pl.ds(i * piece, piece)], x_sem.at[other, i]))
            copies[-1].start()
        return copies

    def wait(copies):
        for copy in copies:
            copy.wait()

    def load_shared(k):
        for i in range(PIECES):
            sent["pair", k, i].wait_recv()
        return load(k, 1)

    def arrive(k):
        for i in range(PIECES):
            sent["ici", k, i].wait_recv()
        for i in range(PIECES):
            for later in range(4, BATCHES):
                if BEFORE[later] == k:
                    send(later, i)
        for i in range(PIECES):
            share(k, i)
        return load(k, 0)

    last = BATCHES - 1
    own_load, shared_load = [], load_shared(0)
    wait(w_copies)
    for k in range(BATCHES):
        compute(k, 0)
        if k == 0:
            wait(kept)
        if k + 1 < last:
            own_load = arrive(k + 1)
        if k == last:
            shared_load = load_shared(k)
        wait(shared_load)
        compute(k, 1)
        if k + 1 == last:
            own_load = arrive(last)
        elif k < last:
            shared_load = load_shared(k + 1)
        for i in range(PIECES):
            part = pl.ds(i * piece, piece)
            first, second = st_s[0, part, :], st_s[1, part, :]
            both = jnp.concatenate(
                [jnp.where(core == 0, first, second), jnp.where(core == 0, second, first)], 0
            ).T
            pair = lax.div(flip(me, 2 * MASKS[i][k]), 2) * PIECES + i
            for t in range(3):
                own_s[t, pl.ds(pair, 1), :] = both[t : t + 1, :]
        if k < last:
            wait(own_load)

    stats = to_all(n, me, own_s, all_s, st_send, st_recv)
    all_s[me] = own_s[...]
    for copy in stats:
        copy.wait_recv()
    high, sums, right = all_s[:, 0], all_s[:, 1], all_s[:, 2]
    top = jnp.max(high, 0)
    total = jnp.sum(sums * jnp.exp(high - top[None]), 0)
    top_ref[...] = top
    inv_ref[...] = 1.0 / total
    loss_ref[...] = jnp.log(total) + top - jnp.sum(right, 0)
    for copy in labels + stats + list(sent.values()):
        copy.wait_send()
    for copies in z_copies.values():
        for copy in copies:
            copy.wait()


def logits_call(n, x, w, lab):
    own, depth = x.shape
    columns = w.shape[1]
    pairs = n // 2 * PIECES
    anywhere, vmem = pl.BlockSpec(memory_space=pl.ANY), pl.BlockSpec(memory_space=pltpu.VMEM)
    dma = pltpu.SemaphoreType.DMA
    return pl.pallas_call(
        functools.partial(logits_kernel, n),
        in_specs=[anywhere, anywhere, vmem],
        out_specs=[anywhere, anywhere, vmem, vmem, vmem, vmem],
        out_shape=[
            jax.ShapeDtypeStruct((BATCHES, 2 * own, depth), BF16),
            jax.ShapeDtypeStruct((BATCHES, 2 * own, columns), F32),
            jax.ShapeDtypeStruct((n,) + lab.shape, jnp.int32),
            jax.ShapeDtypeStruct((pairs, 128), F32),
            jax.ShapeDtypeStruct((pairs, 128), F32),
            jax.ShapeDtypeStruct((pairs, 128), F32),
        ],
        scratch_shapes=[
            pltpu.VMEM((depth, columns), BF16),
            pltpu.VMEM((2, own, depth), BF16),
            pltpu.VMEM((2, own, columns), F32),
            pltpu.VMEM((own, 128), F32),
            pltpu.VMEM((own, 128), F32),
            pltpu.VMEM((own, 128), F32),
            pltpu.VMEM((own, 128), jnp.int32),
            pltpu.VMEM((2, own, 128), F32),
            pltpu.VMEM((3, pairs, 128), F32),
            pltpu.VMEM((n, 3, pairs, 128), F32),
            dma((8,)),
            dma((2, PIECES)),
            dma((PIECES,)),
            dma((2, PIECES)),
            dma((BATCHES, PIECES)),
            dma((BATCHES, PIECES)),
            dma((BATCHES, PIECES)),
            dma((BATCHES, PIECES)),
            dma((n,)),
            dma((n,)),
            dma((n,)),
            dma((n,)),
        ],
        compiler_params=pltpu.CompilerParams(vmem_limit_bytes=VMEM_LIMIT, collective_id=0, has_side_effects=True),
        cost_estimate=pl.CostEstimate(flops=2 * n * own * depth * columns, bytes_accessed=1 << 27, transcendentals=0),
        name="gather_logits",
    )(x, w, lab)


PASSES = tuple((7 - t if t < 8 else None, 8 - t if t > 0 else None) for t in range(9))


def joins(k):
    return tuple(b for b in range(1, BATCHES) if BEFORE[b] == k)


def scatter_kernel(
    n, z_ref, w_ref, x_ref, top_ref, inv_ref, lab_ref,
    out_ref, g_ref, part_ref, took_ref, pass_ref, came_ref,
    z_v, g_v, w_v, in_v, p_v, o_v, last_v, fin_v, top_s, inv_s, off_s, gw_v,
    z_sem, g_sem, w_sem, in_sem, p_sem, o_sem, fin_sem, gw_sem, pair_recv, ici_send, ici_recv,
):
    me = lax.axis_index("tp")
    core = lax.rem(me, 2)
    half = z_ref.shape[1] // 2
    piece = half // PIECES
    depth, columns = w_ref.shape
    wide = w_v.shape[1]
    steps = depth // wide

    groups = [[(k, other) for k, other in ((given, 1), (own, 0)) if k is not None] for given, own in PASSES]
    flat = [group for one in groups for group in one]

    def start(copies):
        for copy in copies:
            copy.start()
        return copies

    def wait(copies):
        for copy in copies:
            copy.wait()

    def load_z(number):
        k, other = flat[number]
        return [
            pltpu.make_async_copy(
                z_ref.at[k, pl.ds(i * 2 * piece + other * piece, piece)],
                z_v.at[number % 2, pl.ds(i * piece, piece)],
                z_sem.at[number % 2, i],
            )
            for i in range(PIECES)
        ]

    def columns_at(j):
        return pl.ds(pl.multiple_of(j * wide, wide), wide)

    def load_w(j, slot):
        return pltpu.make_async_copy(w_ref.at[columns_at(j)], w_v.at[slot], w_sem.at[slot])

    loading = start(load_z(0))
    load_w(0, 0).start()
    meet(n, me)

    lane = lax.broadcasted_iota(jnp.int32, (32, 128), 1)
    sent, load_g = {}, []
    number = 0
    for t, (given, own) in enumerate(PASSES):
        places = {group: place for place, group in enumerate(groups[t])}
        rows = half * len(places)
        g_copies = []
        for (k, other), place in places.items():
            for i in range(PIECES):
                pair = lax.div(flip(me, 2 * MASKS[i][k]), 2) * PIECES + i
                for from_ref, to_ref in ((top_ref, top_s), (inv_ref, inv_s), (lab_ref, off_s)):
                    both = as_column(from_ref[pl.ds(pair, 1), :])
                    to_ref[pl.ds(i * piece, piece), :] = jnp.where(core == other, both[:piece], both[piece:])
            wait(loading)
            slot = number % 2
            number += 1
            if number < len(flat):
                loading = start(load_z(number))

            def body(b, carry, slot=slot, place=place):
                part = pl.ds(pl.multiple_of(b * 32, 32), 32)
                to = pl.ds(pl.multiple_of(place * half + b * 32, 32), 32)
                top, inv, off = top_s[part, :], inv_s[part, :], off_s[part, :].astype(jnp.int32) - lane
                for c in range(0, columns, 128):
                    e = jnp.exp(z_v[slot, part, c : c + 128] - top) * inv
                    g_v[to, c : c + 128] = jnp.where(off == c, e - 1.0, e).astype(BF16)
                return carry

            lax.fori_loop(0, half // 32, body, 0)
            for i in range(PIECES):
                g_copies.append(
                    pltpu.make_async_copy(
                        g_v.at[pl.ds(place * half + i * piece, piece)],
                        g_ref.at[k, pl.ds(i * 2 * piece + other * piece, piece)],
                        g_sem.at[place, i],
                    )
                )
                g_copies[-1].start()

        arrivals = []
        if own is not None:
            pltpu.make_async_remote_copy(
                src_ref=took_ref.at[own],
                dst_ref=took_ref.at[own],
                send_sem=p_sem.at[0],
                recv_sem=pair_recv.at[own],
                device_id={"tp": flip(me, 1)},
                device_id_type=MESH,
            ).wait_recv()
            arrivals.append(took_ref.at[own])
            for b in joins(own) if own else ():
                for i in range(PIECES):
                    sent[b, i].wait_recv()
                arrivals.append(came_ref.at[b])

        def load_in(j, slot, arrivals=arrivals):
            return [
                pltpu.make_async_copy(ref.at[:, columns_at(j)], in_v.at[slot, m], in_sem.at[slot, m])
                for m, ref in enumerate(arrivals)
            ]

        def outs(j, slot, given=given, own=own):
            copies = []
            if given is not None:
                copies.append(
                    pltpu.make_async_remote_copy(
                        src_ref=p_v.at[slot],
                        dst_ref=took_ref.at[given, :, columns_at(j)],
                        send_sem=p_sem.at[slot],
                        recv_sem=pair_recv.at[given],
                        device_id={"tp": flip(me, 1)},
                        device_id_type=MESH,
                    )
                )
            if own:
                copies.append(pltpu.make_async_copy(o_v.at[slot], pass_ref.at[own, :, columns_at(j)], o_sem.at[slot]))
            return copies

        def finished(copies, given=given):
            for m, copy in enumerate(copies):
                if m == 0 and given is not None:
                    copy.wait_send()
                else:
                    copy.wait()

        start(load_in(0, 0))

        def multiply(j, carry, t=t, given=given, own=own, rows=rows, load_in=load_in, outs=outs, finished=finished, count=len(arrivals)):
            slot = lax.rem(j, 2)
            if t < len(PASSES) - 1:
                load_w(lax.rem(j + 1, steps), 1 - slot).start()

            @pl.when(j + 1 < steps)
            def _():
                if t == len(PASSES) - 1:
                    load_w(j + 1, 1 - slot).start()
                start(load_in(j + 1, 1 - slot))

            @pl.when(j > 0)
            def _():
                start(outs(j - 1, 1 - slot))

            @pl.when(j > 1)
            def _():
                finished(outs(j - 2, slot))

            load_w(j, slot).wait()
            wait(load_in(j, slot))
            term = dot(g_v[:rows, :], w_v[slot], ((1,), (1,)))
            if given is not None:
                p_v[slot] = term[:half].astype(BF16)
            if own is not None:
                value = term[rows - half :]
                for m in range(count):
                    value = value + in_v[slot, m].astype(F32)
                if own:
                    o_v[slot] = value.astype(BF16)
                else:
                    last_v[:, columns_at(j)] = value
            return carry

        lax.fori_loop(0, steps, multiply, 0)
        start(outs(steps - 1, (steps - 1) % 2))
        for j in (steps - 2, steps - 1):
            finished(outs(j, j % 2))
        wait(g_copies)
        if own is not None:
            for i in range(PIECES if own else 0):
                part = pl.ds(i * piece, piece)
                sent[own, i] = pltpu.make_async_remote_copy(
                    src_ref=pass_ref.at[own, part],
                    dst_ref=came_ref.at[own, part],
                    send_sem=ici_send.at[own, i],
                    recv_sem=ici_recv.at[own, i],
                    device_id=across(me, i, own),
                    device_id_type=MESH,
                )
                sent[own, i].start()
            load_g += start([pltpu.make_async_copy(g_ref.at[own], gw_v.at[pl.ds(own * 2 * half, 2 * half)], gw_sem.at[own])])

    wait(load_g)

    def outer(x_tile, out_tile):
        out_tile[...] = dot(x_tile[...], gw_v[...], ((0,), (0,))).astype(BF16)

    pltpu.emit_pipeline(
        outer,
        grid=(part_ref.shape[0] // BY_W_TALL,),
        in_specs=[pl.BlockSpec((BATCHES * 2 * half, BY_W_TALL), lambda j: (0, j))],
        out_specs=[pl.BlockSpec((BY_W_TALL, columns), lambda j: (j, 0))],
    )(x_ref, part_ref)

    ends = []
    for m, b in enumerate(reversed(joins(0))):
        for i in range(PIECES):
            sent[b, i].wait_recv()
        ends += start([pltpu.make_async_copy(came_ref.at[b], fin_v.at[m], fin_sem.at[m])])
    wait(ends)

    def finish(j, carry):
        at = columns_at(j)
        value = last_v[:, at]
        for m in range(len(joins(0))):
            value = value + fin_v[m, :, at].astype(F32)
        fin_v[0, :, at] = value.astype(BF16)
        return carry

    lax.fori_loop(0, steps, finish, 0)
    wait(start([pltpu.make_async_copy(fin_v.at[0], out_ref, fin_sem.at[0])]))
    for copy in sent.values():
        copy.wait_send()


def scatter_call(n, z, w, xb, top, inv, lab):
    depth, columns = w.shape
    half, wide = z.shape[1] // 2, 1024
    anywhere, vmem = pl.BlockSpec(memory_space=pl.ANY), pl.BlockSpec(memory_space=pltpu.VMEM)
    dma = pltpu.SemaphoreType.DMA
    moved = jax.ShapeDtypeStruct((BATCHES, half, depth), BF16)
    most = 1 + max(len(joins(k)) for k in range(1, BATCHES))
    return pl.pallas_call(
        functools.partial(scatter_kernel, n),
        in_specs=[anywhere, anywhere, anywhere, vmem, vmem, vmem],
        out_specs=[anywhere] * 6,
        out_shape=[
            jax.ShapeDtypeStruct((half, depth), BF16),
            jax.ShapeDtypeStruct(z.shape, BF16),
            jax.ShapeDtypeStruct((BY_W_EARLY * BY_W_TALL, columns), BF16),
            moved,
            moved,
            moved,
        ],
        scratch_shapes=[
            pltpu.VMEM((2, half, columns), F32),
            pltpu.VMEM((2 * half, columns), BF16),
            pltpu.VMEM((2, wide, columns), BF16),
            pltpu.VMEM((2, most, half, wide), BF16),
            pltpu.VMEM((2, half, wide), BF16),
            pltpu.VMEM((2, half, wide), BF16),
            pltpu.VMEM((half, depth), F32),
            pltpu.VMEM((len(joins(0)), half, depth), BF16),
            pltpu.VMEM((half, 128), F32),
            pltpu.VMEM((half, 128), F32),
            pltpu.VMEM((half, 128), F32),
            pltpu.VMEM((BATCHES * 2 * half, columns), BF16),
            dma((2, PIECES)),
            dma((2, PIECES)),
            dma((2,)),
            dma((2, most)),
            dma((2,)),
            dma((2,)),
            dma((3,)),
            dma((BATCHES,)),
            dma((BATCHES,)),
            dma((BATCHES, PIECES)),
            dma((BATCHES, PIECES)),
        ],
        compiler_params=pltpu.CompilerParams(vmem_limit_bytes=VMEM_LIMIT, collective_id=1, has_side_effects=True),
        cost_estimate=pl.CostEstimate(flops=3 * n * half * depth * columns, bytes_accessed=1 << 28, transcendentals=0),
        name="by_x_scatter",
    )(z, w, xb, top, inv, lab)


def by_w_kernel(x_ref, g_ref, part_ref, out_ref, g_v, part_v, g_sem, part_sem):
    rows, columns = g_ref.shape
    early = part_ref.shape[0]
    g_load = [
        pltpu.make_async_copy(g_ref.at[pl.ds(p * rows // 8, rows // 8)], g_v.at[pl.ds(p * rows // 8, rows // 8)], g_sem.at[p])
        for p in range(8)
    ]
    load = pltpu.make_async_copy(part_ref, part_v, part_sem.at[0])
    for copy in g_load:
        copy.start()
    load.start()
    for copy in g_load:
        copy.wait()

    def outer(x_tile, out_tile):
        out_tile[...] = dot(x_tile[...], g_v[...], ((0,), (0,))).astype(BF16)

    tiles = (out_ref.shape[0] - early) // BY_W_TALL

    def run(first, count):
        skip = early // BY_W_TALL + first
        pltpu.emit_pipeline(
            outer,
            grid=(count,),
            in_specs=[pl.BlockSpec((rows, BY_W_TALL), lambda j: (0, skip + j))],
            out_specs=[pl.BlockSpec((BY_W_TALL, columns), lambda j: (skip + j, 0))],
        )(x_ref, out_ref)

    run(0, tiles // 2)
    load.wait()
    store = pltpu.make_async_copy(part_v, out_ref.at[pl.ds(0, early)], part_sem.at[1])
    store.start()
    run(tiles // 2, tiles - tiles // 2)
    store.wait()


def by_w_call(xb, g, part):
    rows, depth = xb.shape
    columns = g.shape[1]
    anywhere = pl.BlockSpec(memory_space=pl.ANY)
    dma = pltpu.SemaphoreType.DMA
    return pl.pallas_call(
        by_w_kernel,
        in_specs=[anywhere] * 3,
        out_specs=anywhere,
        out_shape=jax.ShapeDtypeStruct((depth, columns), BF16),
        scratch_shapes=[pltpu.VMEM((rows, columns), BF16), pltpu.VMEM(part.shape, BF16), dma((8,)), dma((2,))],
        compiler_params=pltpu.CompilerParams(vmem_limit_bytes=VMEM_LIMIT),
        cost_estimate=pl.CostEstimate(flops=rows * depth * columns, bytes_accessed=1 << 26, transcendentals=0),
        name="by_w",
    )(xb, g, part)


def solution(mesh):
    n = mesh.shape["tp"]

    def step(x, w, label):
        me, own, columns = lax.axis_index("tp"), x.shape[0], w.shape[1]
        piece = own // PIECES
        lab = jnp.pad(label.reshape(PIECES, piece), ((0, 0), (0, 128 - piece)))
        xb, z, labs, top, inv, loss = logits_call(n, x, w, lab)
        mine = labs[:, :, :piece].reshape(n // 2, 2, PIECES, piece).swapaxes(1, 2).reshape(-1, 128) - me * columns
        by_x, g, part, *_ = scatter_call(n, z, w, xb.reshape(-1, xb.shape[-1]), top, inv, mine.astype(F32))
        by_w = by_w_call(xb.reshape(-1, xb.shape[-1]), g.reshape(-1, columns), part)
        by_device = loss.reshape(n // 2, PIECES, 2, piece).swapaxes(1, 2).reshape(n, own)
        return lax.dynamic_index_in_dim(by_device, me, 0, keepdims=False), by_x, by_w

    return jax.shard_map(
        step,
        mesh=mesh,
        in_specs=(P(("dp", "tp"), None), P(None, "tp"), P(("dp", "tp"))),
        out_specs=(P(("dp", "tp")), P(("dp", "tp"), None), P("dp", "tp")),
        check_vma=False,
    )
```

```python
import functools

import jax
import jax.numpy as jnp
from jax import lax
from jax.experimental import pallas as pl
from jax.experimental.pallas import tpu as pltpu
from jax.sharding import PartitionSpec as P

F32, BF16 = jnp.float32, jnp.bfloat16
MESH = pl.DeviceIdType.MESH
VMEM_LIMIT = 63 * 1024 * 1024

ORDERS = ((4, 2, 1), (2, 1, 4), (1, 4, 2))
LAST = (None, 0, 1, 1, 2, 2, 2, 2)
BEFORE = (None, 0, 0, 1, 0, 1, 2, 3)
BATCHES, PIECES = 8, 3
BY_W_TALL = 256
BY_W_EARLY = 10


def dot(a, b, contract):
    return lax.dot_general(a, b, (contract, ((), ())), preferred_element_type=F32)


def flip(index, mask):
    for bit in (1, 2, 4, 8):
        if mask & bit:
            index = index + bit - 2 * bit * lax.rem(lax.div(index, bit), 2)
    return index


def source_of(me, k, i):
    index = me
    for bit, on in zip(ORDERS[i], (lax.rem(k, 2), lax.rem(lax.div(k, 2), 2), lax.div(k, 4))):
        index = index + on * (2 * bit) * (1 - 2 * lax.rem(lax.div(me, 2 * bit), 2))
    return index


def across(me, i, k):
    return {"tp": flip(me, 2 * ORDERS[i][LAST[k]])}


def meet(n, me):
    barrier = pltpu.get_barrier_semaphore()
    for j in range(1, n):
        pl.semaphore_signal(barrier, inc=1, device_id={"tp": lax.rem(me + j, n)}, device_id_type=MESH)
    pl.semaphore_wait(barrier, n - 1)


def all_copy(n, me, own_ref, all_ref, send_sems, recv_sems, j):
    return pltpu.make_async_remote_copy(
        src_ref=own_ref,
        dst_ref=all_ref.at[me],
        send_sem=send_sems.at[j],
        recv_sem=recv_sems.at[j],
        device_id={"tp": lax.rem(me + j, n)},
        device_id_type=MESH,
    )


def to_all(n, me, own_ref, all_ref, send_sems, recv_sems):
    copies = [all_copy(n, me, own_ref, all_ref, send_sems, recv_sems, j) for j in range(1, n)]
    for copy in copies:
        copy.start()
    return copies


def as_column(row):
    return jnp.broadcast_to(row, (128, 128)).T


def logits_kernel(
    n, x_ref, w_ref, lab_ref, xb_ref, z_ref, rel_ref, top_ref, inv_ref, loss_ref,
    w_v, x_v, z_v, m_s, s_s, r_s, off_s, st_s, own_s, all_s, end_s, ends_s, labs_s,
    w_sem, x_sem, keep_sem, z_sem, ici_send, ici_recv, pair_send, pair_recv, lab_send, lab_recv, st_send, st_recv,
    end_send, end_recv,
):
    me = lax.axis_index("tp")
    core = lax.rem(me, 2)
    piece = x_ref.shape[0] // PIECES
    half = PIECES * piece
    depth, columns = w_ref.shape
    wide = 1024
    last = BATCHES - 1

    def start(copies):
        for copy in copies:
            copy.start()
        return copies

    def wait(copies):
        for copy in copies:
            copy.wait()

    w_parts = 8
    w_copies = []
    for p in range(w_parts):
        part = pl.ds(p * (depth // w_parts), depth // w_parts)
        w_copies.append(pltpu.make_async_copy(w_ref.at[part], w_v.at[part], w_sem.at[p]))
    x_load = pltpu.make_async_copy(x_ref, x_v.at[0], x_sem.at[0, 0])
    start([x_load] + w_copies)
    own_s[...] = jnp.zeros(own_s.shape, F32)
    end_s[...] = jnp.zeros(end_s.shape, F32)

    meet(n, me)

    def slot(k, i, other):
        return xb_ref.at[k, pl.ds(i * 2 * piece + other * piece, piece)]

    def source(k, i):
        return x_ref.at[pl.ds(i * piece, piece)] if k == 0 else slot(k, i, 0)

    def send(k, i):
        return pltpu.make_async_remote_copy(
            src_ref=source(BEFORE[k], i),
            dst_ref=slot(k, i, 0),
            send_sem=ici_send.at[k, i],
            recv_sem=ici_recv.at[k, i],
            device_id=across(me, i, k),
            device_id_type=MESH,
        )

    def share(k, i, from_x=False):
        return pltpu.make_async_remote_copy(
            src_ref=source(0, i) if from_x else slot(k, i, 0),
            dst_ref=slot(k, i, 1),
            send_sem=pair_send.at[k, i],
            recv_sem=pair_recv.at[k, i],
            device_id={"tp": flip(me, 1)},
            device_id_type=MESH,
        )

    labels = to_all(n, me, lab_ref, labs_s, lab_send, lab_recv)
    start([send(1, i) for i in range(PIECES)])
    start([share(0, i, True) for i in range(PIECES)])
    for k in (2, 4):
        start([send(k, i) for i in range(PIECES)])
    labs_s[me] = lab_ref[...]
    x_load.wait()
    kept = start(
        [pltpu.make_async_copy(x_v.at[0, pl.ds(i * piece, piece)], slot(0, i, 0), keep_sem.at[i]) for i in range(PIECES)]
    )
    for copy in labels:
        copy.wait_recv()
    low = lax.broadcasted_iota(jnp.int32, (1, 128), 1) < piece
    for chip in range(n // 2):
        for i in range(PIECES):
            first, second = labs_s[2 * chip, i : i + 1, :].astype(F32), labs_s[2 * chip + 1, i : i + 1, :].astype(F32)
            rel_ref[chip * PIECES + i : chip * PIECES + i + 1, :] = (
                jnp.where(low, first, pltpu.roll(second, piece, 1)) - (me * columns).astype(F32)
            )

    lane = lax.broadcasted_iota(jnp.int32, (half, 128), 1)

    def load(k, other):
        return [
            pltpu.make_async_copy(slot(k, i, other), x_v.at[other, pl.ds(i * piece, piece)], x_sem.at[other, i])
            for i in range(PIECES)
        ]

    def store_z(k, other):
        return [
            pltpu.make_async_copy(
                z_v.at[other, pl.ds(i * piece, piece)],
                z_ref.at[k, pl.ds(i * 2 * piece + other * piece, piece)],
                z_sem.at[other, i],
            )
            for i in range(PIECES)
        ]

    def compute(k, other):
        for i in range(PIECES):
            dev = source_of(me, k, i)
            dev = flip(dev, 1) if other else dev
            row = (labs_s[dev, pl.ds(i, 1), :] - me * columns).astype(F32)
            off_s[pl.ds(i * piece, piece), :] = as_column(row)[:piece].astype(jnp.int32)
        m_s[...] = jnp.full(m_s.shape, -jnp.inf, F32)
        s_s[...] = jnp.zeros(s_s.shape, F32)
        r_s[...] = jnp.zeros(r_s.shape, F32)

        @pl.when(k > 0)
        def _():
            wait(store_z(k, other))

        def body(j, carry):
            at = pl.multiple_of(j * wide, wide)
            z = dot(x_v[other], w_v[:, pl.ds(at, wide)], ((1,), (0,)))
            z_v[other, :, pl.ds(at, wide)] = z
            old = m_s[...]
            new = old
            for c in range(0, wide, 128):
                new = jnp.maximum(new, z[:, c : c + 128])
            total = s_s[...] * jnp.exp(old - new)
            right = r_s[...]
            off = off_s[...] - at
            for c in range(0, wide, 128):
                total += jnp.exp(z[:, c : c + 128] - new)
                right += jnp.where(lane == off - c, z[:, c : c + 128], 0.0)
            m_s[...] = new
            s_s[...] = total
            r_s[...] = right
            return carry

        lax.fori_loop(0, columns // wide, body, 0)
        start(store_z(k, other))
        high = jnp.max(m_s[...], -1, keepdims=True)
        total = jnp.sum(s_s[...] * jnp.exp(m_s[...] - high), -1, keepdims=True)
        right = jnp.sum(r_s[...], -1, keepdims=True)
        st_s[other] = jnp.where(lane == 0, high, jnp.where(lane == 1, total, jnp.where(lane == 2, right, 0.0)))

    def arrive(k):
        for i in range(PIECES):
            send(k, i).wait_recv()
        start([send(later, i) for i in range(PIECES) for later in range(1, BATCHES) if BEFORE[later] == k])
        start([share(k, i) for i in range(PIECES)])
        start(load(k, 0))

    def load_shared(k):
        for i in range(PIECES):
            share(k, i).wait_recv()
        start(load(k, 1))

    load_shared(0)
    wait(w_copies)

    def batch(k, carry):
        compute(k, 0)

        @pl.when(k == 0)
        def _():
            wait(kept)

        for now in range(1, last):

            @pl.when(k + 1 == now)
            def _(now=now):
                arrive(now)

        @pl.when(k == last)
        def _():
            to_all(n, me, own_s, all_s, st_send, st_recv)
            load_shared(last)

        wait(load(k, 1))
        compute(k, 1)

        @pl.when(k + 1 == last)
        def _():
            arrive(last)

        @pl.when(k + 1 < last)
        def _():
            load_shared(k + 1)

        for i in range(PIECES):
            part = pl.ds(i * piece, piece)
            first, second = st_s[0, part, :], st_s[1, part, :]
            both = jnp.concatenate(
                [jnp.where(core == 0, first, second), jnp.where(core == 0, second, first)], 0
            ).T
            pair = lax.div(source_of(me, k, i), 2) * PIECES + i

            @pl.when(k < last)
            def _(i=i, both=both, pair=pair):
                for t in range(3):
                    own_s[t, pl.ds(pair, 1), :] = both[t : t + 1, :]

            @pl.when(k == last)
            def _(i=i, both=both):
                for t in range(3):
                    end_s[t, i : i + 1, :] = both[t : t + 1, :]

        @pl.when(k < last)
        def _():
            wait(load(k + 1, 0))

        return carry

    lax.fori_loop(0, BATCHES, batch, 0)

    all_s[me] = own_s[...]
    ends_s[me] = end_s[...]
    ends = to_all(n, me, end_s, ends_s, end_send, end_recv)
    stats = [all_copy(n, me, own_s, all_s, st_send, st_recv, j) for j in range(1, n)]
    for copy in stats + ends:
        copy.wait_recv()
    for dev in range(n):
        row = (n // 2 - 1 - dev // 2) * PIECES
        for t in range(3):
            all_s[dev, t, row : row + PIECES, :] = ends_s[dev, t, :PIECES, :]
    high, sums, right = all_s[:, 0], all_s[:, 1], all_s[:, 2]
    top = jnp.max(high, 0)
    total = jnp.sum(sums * jnp.exp(high - top[None]), 0)
    top_ref[...] = top
    inv_ref[...] = 1.0 / total
    loss_ref[...] = jnp.log(total) + top - jnp.sum(right, 0)
    for copy in labels + stats + ends:
        copy.wait_send()
    for k in range(BATCHES):
        for i in range(PIECES):
            share(k, i, k == 0).wait_send()
            if k > 0:
                send(k, i).wait_send()
    wait(store_z(last, 0) + store_z(last, 1))


def logits_call(n, x, w, lab):
    own, depth = x.shape
    columns = w.shape[1]
    pairs = n // 2 * PIECES
    anywhere, vmem = pl.BlockSpec(memory_space=pl.ANY), pl.BlockSpec(memory_space=pltpu.VMEM)
    dma = pltpu.SemaphoreType.DMA
    return pl.pallas_call(
        functools.partial(logits_kernel, n),
        in_specs=[anywhere, anywhere, vmem],
        out_specs=[anywhere, anywhere, vmem, vmem, vmem, vmem],
        out_shape=[
            jax.ShapeDtypeStruct((BATCHES, 2 * own, depth), BF16),
            jax.ShapeDtypeStruct((BATCHES, 2 * own, columns), F32),
            jax.ShapeDtypeStruct((pairs, 128), F32),
            jax.ShapeDtypeStruct((pairs, 128), F32),
            jax.ShapeDtypeStruct((pairs, 128), F32),
            jax.ShapeDtypeStruct((pairs, 128), F32),
        ],
        scratch_shapes=[
            pltpu.VMEM((depth, columns), BF16),
            pltpu.VMEM((2, own, depth), BF16),
            pltpu.VMEM((2, own, columns), F32),
            pltpu.VMEM((own, 128), F32),
            pltpu.VMEM((own, 128), F32),
            pltpu.VMEM((own, 128), F32),
            pltpu.VMEM((own, 128), jnp.int32),
            pltpu.VMEM((2, own, 128), F32),
            pltpu.VMEM((3, pairs, 128), F32),
            pltpu.VMEM((n, 3, pairs, 128), F32),
            pltpu.VMEM((3, 8, 128), F32),
            pltpu.VMEM((n, 3, 8, 128), F32),
            pltpu.VMEM((n,) + lab.shape, jnp.int32),
            dma((8,)),
            dma((2, PIECES)),
            dma((PIECES,)),
            dma((2, PIECES)),
            dma((BATCHES, PIECES)),
            dma((BATCHES, PIECES)),
            dma((BATCHES, PIECES)),
            dma((BATCHES, PIECES)),
            dma((n,)),
            dma((n,)),
            dma((n,)),
            dma((n,)),
            dma((n,)),
            dma((n,)),
        ],
        compiler_params=pltpu.CompilerParams(vmem_limit_bytes=VMEM_LIMIT, collective_id=0, has_side_effects=True),
        cost_estimate=pl.CostEstimate(flops=2 * n * own * depth * columns, bytes_accessed=1 << 27, transcendentals=0),
        name="gather_logits",
    )(x, w, lab)


PASSES = tuple((7 - t if t < 8 else None, 8 - t if t > 0 else None) for t in range(9))


def joins(k):
    return tuple(b for b in range(1, BATCHES) if BEFORE[b] == k)


def scatter_kernel(
    n, z_ref, w_ref, x_ref, top_ref, inv_ref, lab_ref,
    out_ref, g_ref, part_ref, took_ref, pass_ref, came_ref,
    z_v, g_v, w_v, in_v, p_v, o_v, last_v, fin_v, top_s, inv_s, off_s, gw_v,
    z_sem, g_sem, w_sem, in_sem, p_sem, o_sem, fin_sem, gw_sem, pair_recv, ici_send, ici_recv,
):
    me = lax.axis_index("tp")
    core = lax.rem(me, 2)
    half = z_ref.shape[1] // 2
    piece = half // PIECES
    depth, columns = w_ref.shape
    wide = w_v.shape[1]
    steps = depth // wide

    groups = [[(k, other) for k, other in ((given, 1), (own, 0)) if k is not None] for given, own in PASSES]
    flat = [group for one in groups for group in one]

    def start(copies):
        for copy in copies:
            copy.start()
        return copies

    def wait(copies):
        for copy in copies:
            copy.wait()

    def load_z(number):
        k, other = flat[number]
        return [
            pltpu.make_async_copy(
                z_ref.at[k, pl.ds(i * 2 * piece + other * piece, piece)],
                z_v.at[number % 2, pl.ds(i * piece, piece)],
                z_sem.at[number % 2, i],
            )
            for i in range(PIECES)
        ]

    def columns_at(j):
        return pl.ds(pl.multiple_of(j * wide, wide), wide)

    def load_w(j, slot):
        return pltpu.make_async_copy(w_ref.at[columns_at(j)], w_v.at[slot], w_sem.at[slot])

    loading = start(load_z(0))
    load_w(0, 0).start()
    meet(n, me)

    lane = lax.broadcasted_iota(jnp.int32, (32, 128), 1)
    sent, load_g = {}, []
    number = 0
    for t, (given, own) in enumerate(PASSES):
        places = {group: place for place, group in enumerate(groups[t])}
        rows = half * len(places)
        g_copies = []
        for (k, other), place in places.items():
            for i in range(PIECES):
                pair = lax.div(source_of(me, jnp.int32(k), i), 2) * PIECES + i
                for from_ref, to_ref in ((top_ref, top_s), (inv_ref, inv_s), (lab_ref, off_s)):
                    both = as_column(from_ref[pl.ds(pair, 1), :])
                    to_ref[pl.ds(i * piece, piece), :] = jnp.where(core == other, both[:piece], both[piece:])
            wait(loading)
            slot = number % 2
            number += 1
            if number < len(flat):
                loading = start(load_z(number))

            def body(b, carry, slot=slot, place=place):
                part = pl.ds(pl.multiple_of(b * 32, 32), 32)
                to = pl.ds(pl.multiple_of(place * half + b * 32, 32), 32)
                top, inv, off = top_s[part, :], inv_s[part, :], off_s[part, :].astype(jnp.int32) - lane
                for c in range(0, columns, 128):
                    e = jnp.exp(z_v[slot, part, c : c + 128] - top) * inv
                    g_v[to, c : c + 128] = jnp.where(off == c, e - 1.0, e).astype(BF16)
                return carry

            lax.fori_loop(0, half // 32, body, 0)
            for i in range(PIECES):
                g_copies.append(
                    pltpu.make_async_copy(
                        g_v.at[pl.ds(place * half + i * piece, piece)],
                        g_ref.at[k, pl.ds(i * 2 * piece + other * piece, piece)],
                        g_sem.at[place, i],
                    )
                )
                g_copies[-1].start()

        arrivals = []
        if own is not None:
            pltpu.make_async_remote_copy(
                src_ref=took_ref.at[own],
                dst_ref=took_ref.at[own],
                send_sem=p_sem.at[0],
                recv_sem=pair_recv.at[own],
                device_id={"tp": flip(me, 1)},
                device_id_type=MESH,
            ).wait_recv()
            arrivals.append(took_ref.at[own])
            for b in joins(own) if own else ():
                for i in range(PIECES):
                    sent[b, i].wait_recv()
                arrivals.append(came_ref.at[b])

        def load_in(j, slot, arrivals=arrivals):
            return [
                pltpu.make_async_copy(ref.at[:, columns_at(j)], in_v.at[slot, m], in_sem.at[slot, m])
                for m, ref in enumerate(arrivals)
            ]

        def outs(j, slot, given=given, own=own):
            copies = []
            if given is not None:
                copies.append(
                    pltpu.make_async_remote_copy(
                        src_ref=p_v.at[slot],
                        dst_ref=took_ref.at[given, :, columns_at(j)],
                        send_sem=p_sem.at[slot],
                        recv_sem=pair_recv.at[given],
                        device_id={"tp": flip(me, 1)},
                        device_id_type=MESH,
                    )
                )
            if own:
                copies.append(pltpu.make_async_copy(o_v.at[slot], pass_ref.at[own, :, columns_at(j)], o_sem.at[slot]))
            return copies

        def finished(copies, given=given):
            for m, copy in enumerate(copies):
                if m == 0 and given is not None:
                    copy.wait_send()
                else:
                    copy.wait()

        start(load_in(0, 0))

        def multiply(j, carry, t=t, given=given, own=own, rows=rows, load_in=load_in, outs=outs, finished=finished, count=len(arrivals)):
            slot = lax.rem(j, 2)
            if t < len(PASSES) - 1:
                load_w(lax.rem(j + 1, steps), 1 - slot).start()

            @pl.when(j + 1 < steps)
            def _():
                if t == len(PASSES) - 1:
                    load_w(j + 1, 1 - slot).start()
                start(load_in(j + 1, 1 - slot))

            @pl.when(j > 0)
            def _():
                start(outs(j - 1, 1 - slot))

            @pl.when(j > 1)
            def _():
                finished(outs(j - 2, slot))

            load_w(j, slot).wait()
            wait(load_in(j, slot))
            term = dot(g_v[:rows, :], w_v[slot], ((1,), (1,)))
            if given is not None:
                p_v[slot] = term[:half].astype(BF16)
            if own is not None:
                value = term[rows - half :]
                for m in range(count):
                    value = value + in_v[slot, m].astype(F32)
                if own:
                    o_v[slot] = value.astype(BF16)
                else:
                    last_v[:, columns_at(j)] = value
            return carry

        lax.fori_loop(0, steps, multiply, 0)
        start(outs(steps - 1, (steps - 1) % 2))
        for j in (steps - 2, steps - 1):
            finished(outs(j, j % 2))
        wait(g_copies)
        if own is not None:
            for i in range(PIECES if own else 0):
                part = pl.ds(i * piece, piece)
                sent[own, i] = pltpu.make_async_remote_copy(
                    src_ref=pass_ref.at[own, part],
                    dst_ref=came_ref.at[own, part],
                    send_sem=ici_send.at[own, i],
                    recv_sem=ici_recv.at[own, i],
                    device_id=across(me, i, own),
                    device_id_type=MESH,
                )
                sent[own, i].start()
            load_g += start([pltpu.make_async_copy(g_ref.at[own], gw_v.at[pl.ds(own * 2 * half, 2 * half)], gw_sem.at[own])])

    wait(load_g)

    def outer(x_tile, out_tile):
        out_tile[...] = dot(x_tile[...], gw_v[...], ((0,), (0,))).astype(BF16)

    pltpu.emit_pipeline(
        outer,
        grid=(part_ref.shape[0] // BY_W_TALL,),
        in_specs=[pl.BlockSpec((BATCHES * 2 * half, BY_W_TALL), lambda j: (0, j))],
        out_specs=[pl.BlockSpec((BY_W_TALL, columns), lambda j: (j, 0))],
    )(x_ref, part_ref)

    ends = []
    for m, b in enumerate(reversed(joins(0))):
        for i in range(PIECES):
            sent[b, i].wait_recv()
        ends += start([pltpu.make_async_copy(came_ref.at[b], fin_v.at[m], fin_sem.at[m])])
    wait(ends)

    def finish(j, carry):
        at = columns_at(j)
        value = last_v[:, at]
        for m in range(len(joins(0))):
            value = value + fin_v[m, :, at].astype(F32)
        fin_v[0, :, at] = value.astype(BF16)
        return carry

    lax.fori_loop(0, steps, finish, 0)
    wait(start([pltpu.make_async_copy(fin_v.at[0], out_ref, fin_sem.at[0])]))
    for copy in sent.values():
        copy.wait_send()


def scatter_call(n, z, w, xb, top, inv, lab):
    depth, columns = w.shape
    half, wide = z.shape[1] // 2, 1024
    anywhere, vmem = pl.BlockSpec(memory_space=pl.ANY), pl.BlockSpec(memory_space=pltpu.VMEM)
    dma = pltpu.SemaphoreType.DMA
    moved = jax.ShapeDtypeStruct((BATCHES, half, depth), BF16)
    most = 1 + max(len(joins(k)) for k in range(1, BATCHES))
    return pl.pallas_call(
        functools.partial(scatter_kernel, n),
        in_specs=[anywhere, anywhere, anywhere, vmem, vmem, vmem],
        out_specs=[anywhere] * 6,
        out_shape=[
            jax.ShapeDtypeStruct((half, depth), BF16),
            jax.ShapeDtypeStruct(z.shape, BF16),
            jax.ShapeDtypeStruct((BY_W_EARLY * BY_W_TALL, columns), BF16),
            moved,
            moved,
            moved,
        ],
        scratch_shapes=[
            pltpu.VMEM((2, half, columns), F32),
            pltpu.VMEM((2 * half, columns), BF16),
            pltpu.VMEM((2, wide, columns), BF16),
            pltpu.VMEM((2, most, half, wide), BF16),
            pltpu.VMEM((2, half, wide), BF16),
            pltpu.VMEM((2, half, wide), BF16),
            pltpu.VMEM((half, depth), F32),
            pltpu.VMEM((len(joins(0)), half, depth), BF16),
            pltpu.VMEM((half, 128), F32),
            pltpu.VMEM((half, 128), F32),
            pltpu.VMEM((half, 128), F32),
            pltpu.VMEM((BATCHES * 2 * half, columns), BF16),
            dma((2, PIECES)),
            dma((2, PIECES)),
            dma((2,)),
            dma((2, most)),
            dma((2,)),
            dma((2,)),
            dma((3,)),
            dma((BATCHES,)),
            dma((BATCHES,)),
            dma((BATCHES, PIECES)),
            dma((BATCHES, PIECES)),
        ],
        compiler_params=pltpu.CompilerParams(vmem_limit_bytes=VMEM_LIMIT, collective_id=1, has_side_effects=True),
        cost_estimate=pl.CostEstimate(flops=3 * n * half * depth * columns, bytes_accessed=1 << 28, transcendentals=0),
        name="by_x_scatter",
    )(z, w, xb, top, inv, lab)


def by_w_kernel(x_ref, g_ref, part_ref, by_x_ref, out_ref, by_x_out_ref, g_v, part_v, by_x_v, g_sem, part_sem):
    rows, columns = g_ref.shape
    early = part_ref.shape[0]
    g_load = [
        pltpu.make_async_copy(g_ref.at[pl.ds(p * rows // 8, rows // 8)], g_v.at[pl.ds(p * rows // 8, rows // 8)], g_sem.at[p])
        for p in range(8)
    ]
    load = pltpu.make_async_copy(part_ref, part_v, part_sem.at[0])
    for copy in g_load:
        copy.start()
    load.start()
    by_x_load = pltpu.make_async_copy(by_x_ref, by_x_v, part_sem.at[2])
    by_x_load.start()
    for copy in g_load:
        copy.wait()

    def outer(x_tile, out_tile):
        out_tile[...] = dot(x_tile[...], g_v[...], ((0,), (0,))).astype(BF16)

    tiles = (out_ref.shape[0] - early) // BY_W_TALL

    def run(first, count):
        skip = early // BY_W_TALL + first
        pltpu.emit_pipeline(
            outer,
            grid=(count,),
            in_specs=[pl.BlockSpec((rows, BY_W_TALL), lambda j: (0, skip + j))],
            out_specs=[pl.BlockSpec((BY_W_TALL, columns), lambda j: (skip + j, 0))],
        )(x_ref, out_ref)

    run(0, tiles // 2)
    load.wait()
    store = pltpu.make_async_copy(part_v, out_ref.at[pl.ds(0, early)], part_sem.at[1])
    store.start()
    by_x_load.wait()
    by_x_store = pltpu.make_async_copy(by_x_v, by_x_out_ref, part_sem.at[3])
    by_x_store.start()
    run(tiles // 2, tiles - tiles // 2)
    store.wait()
    by_x_store.wait()


def by_w_call(xb, g, part, by_x):
    rows, depth = xb.shape
    columns = g.shape[1]
    anywhere = pl.BlockSpec(memory_space=pl.ANY)
    dma = pltpu.SemaphoreType.DMA
    return pl.pallas_call(
        by_w_kernel,
        in_specs=[anywhere] * 4,
        out_specs=[anywhere] * 2,
        out_shape=[jax.ShapeDtypeStruct((depth, columns), BF16), jax.ShapeDtypeStruct(by_x.shape, BF16)],
        scratch_shapes=[
            pltpu.VMEM((rows, columns), BF16),
            pltpu.VMEM(part.shape, BF16),
            pltpu.VMEM(by_x.shape, BF16),
            dma((8,)),
            dma((4,)),
        ],
        compiler_params=pltpu.CompilerParams(vmem_limit_bytes=VMEM_LIMIT),
        cost_estimate=pl.CostEstimate(flops=rows * depth * columns, bytes_accessed=1 << 26, transcendentals=0),
        name="by_w",
    )(xb, g, part, by_x)


def solution(mesh):
    n = mesh.shape["tp"]

    def step(x, w, label):
        me, own, columns = lax.axis_index("tp"), x.shape[0], w.shape[1]
        piece = own // PIECES
        lab = jnp.pad(label.reshape(PIECES, piece), ((0, 0), (0, 128 - piece)))
        xb, z, rel, top, inv, loss = logits_call(n, x, w, lab)
        by_x, g, part, *_ = scatter_call(n, z, w, xb.reshape(-1, xb.shape[-1]), top, inv, rel)
        by_w, by_x = by_w_call(xb.reshape(-1, xb.shape[-1]), g.reshape(-1, columns), part, by_x)
        by_device = loss.reshape(n // 2, PIECES, 2, piece).swapaxes(1, 2).reshape(n, own)
        return lax.dynamic_index_in_dim(by_device, me, 0, keepdims=False), by_x, by_w

    return jax.shard_map(
        step,
        mesh=mesh,
        in_specs=(P(("dp", "tp"), None), P(None, "tp"), P(("dp", "tp"))),
        out_specs=(P(("dp", "tp")), P(("dp", "tp"), None), P("dp", "tp")),
        check_vma=False,
    )
```

```python
import functools

import jax
import jax.numpy as jnp
from jax import lax
from jax.experimental import pallas as pl
from jax.experimental.pallas import tpu as pltpu
from jax.sharding import PartitionSpec as P

F32, BF16 = jnp.float32, jnp.bfloat16
MESH = pl.DeviceIdType.MESH
VMEM_LIMIT = 63 * 1024 * 1024

ORDERS = ((4, 2, 1), (2, 1, 4), (1, 4, 2))
LAST = (None, 0, 1, 1, 2, 2, 2, 2)
BEFORE = (None, 0, 0, 1, 0, 1, 2, 3)
BATCHES, PIECES = 8, 3
BY_W_TALL = 256
BY_W_EARLY = 10


def dot(a, b, contract):
    return lax.dot_general(a, b, (contract, ((), ())), preferred_element_type=F32)


def flip(index, mask):
    for bit in (1, 2, 4, 8):
        if mask & bit:
            index = index + bit - 2 * bit * lax.rem(lax.div(index, bit), 2)
    return index


def source_of(me, k, i):
    index = me
    for bit, on in zip(ORDERS[i], (lax.rem(k, 2), lax.rem(lax.div(k, 2), 2), lax.div(k, 4))):
        index = index + on * (2 * bit) * (1 - 2 * lax.rem(lax.div(me, 2 * bit), 2))
    return index


def across(me, i, k):
    return {"tp": flip(me, 2 * ORDERS[i][LAST[k]])}


def meet(n, me):
    barrier = pltpu.get_barrier_semaphore()
    for j in range(1, n):
        pl.semaphore_signal(barrier, inc=1, device_id={"tp": lax.rem(me + j, n)}, device_id_type=MESH)
    pl.semaphore_wait(barrier, n - 1)


def all_copy(n, me, own_ref, all_ref, send_sems, recv_sems, j):
    return pltpu.make_async_remote_copy(
        src_ref=own_ref,
        dst_ref=all_ref.at[me],
        send_sem=send_sems.at[j],
        recv_sem=recv_sems.at[j],
        device_id={"tp": lax.rem(me + j, n)},
        device_id_type=MESH,
    )


def to_all(n, me, own_ref, all_ref, send_sems, recv_sems):
    copies = [all_copy(n, me, own_ref, all_ref, send_sems, recv_sems, j) for j in range(1, n)]
    for copy in copies:
        copy.start()
    return copies


def as_column(row):
    return jnp.broadcast_to(row, (128, 128)).T


def logits_kernel(
    n, x_ref, w_ref, lab_ref, xb_ref, z_ref, rel_ref, top_ref, inv_ref, loss_ref,
    w_v, x_v, z_v, m_s, s_s, r_s, off_s, st_s, own_s, all_s, end_s, ends_s, labs_s,
    w_sem, x_sem, keep_sem, z_sem, ici_send, ici_recv, pair_send, pair_recv, lab_send, lab_recv, st_send, st_recv,
    end_send, end_recv,
):
    me = lax.axis_index("tp")
    core = lax.rem(me, 2)
    piece = x_ref.shape[0] // PIECES
    half = PIECES * piece
    depth, columns = w_ref.shape
    wide = 1024
    last = BATCHES - 1

    def start(copies):
        for copy in copies:
            copy.start()
        return copies

    def wait(copies):
        for copy in copies:
            copy.wait()

    w_parts = 8
    w_copies = []
    for p in range(w_parts):
        part = pl.ds(p * (depth // w_parts), depth // w_parts)
        w_copies.append(pltpu.make_async_copy(w_ref.at[part], w_v.at[part], w_sem.at[p]))
    x_load = pltpu.make_async_copy(x_ref, x_v.at[0], x_sem.at[0, 0])
    start([x_load] + w_copies)
    own_s[...] = jnp.zeros(own_s.shape, F32)
    end_s[...] = jnp.zeros(end_s.shape, F32)

    meet(n, me)

    def slot(k, i, other):
        return xb_ref.at[k, pl.ds(i * 2 * piece + other * piece, piece)]

    def source(k, i):
        return x_ref.at[pl.ds(i * piece, piece)] if k == 0 else slot(k, i, 0)

    def send(k, i):
        return pltpu.make_async_remote_copy(
            src_ref=source(BEFORE[k], i),
            dst_ref=slot(k, i, 0),
            send_sem=ici_send.at[k, i],
            recv_sem=ici_recv.at[k, i],
            device_id=across(me, i, k),
            device_id_type=MESH,
        )

    def share(k, i, from_x=False):
        return pltpu.make_async_remote_copy(
            src_ref=source(0, i) if from_x else slot(k, i, 0),
            dst_ref=slot(k, i, 1),
            send_sem=pair_send.at[k, i],
            recv_sem=pair_recv.at[k, i],
            device_id={"tp": flip(me, 1)},
            device_id_type=MESH,
        )

    labels = to_all(n, me, lab_ref, labs_s, lab_send, lab_recv)
    start([send(1, i) for i in range(PIECES)])
    start([share(0, i, True) for i in range(PIECES)])
    start([send(2, i) for i in range(PIECES)])
    labs_s[me] = lab_ref[...]
    x_load.wait()
    kept = start(
        [pltpu.make_async_copy(x_v.at[0, pl.ds(i * piece, piece)], slot(0, i, 0), keep_sem.at[i]) for i in range(PIECES)]
    )
    for copy in labels:
        copy.wait_recv()
    low = lax.broadcasted_iota(jnp.int32, (1, 128), 1) < piece
    for chip in range(n // 2):
        for i in range(PIECES):
            first, second = labs_s[2 * chip, i : i + 1, :].astype(F32), labs_s[2 * chip + 1, i : i + 1, :].astype(F32)
            rel_ref[chip * PIECES + i : chip * PIECES + i + 1, :] = (
                jnp.where(low, first, pltpu.roll(second, piece, 1)) - (me * columns).astype(F32)
            )

    lane = lax.broadcasted_iota(jnp.int32, (half, 128), 1)

    def load(k, other):
        return [
            pltpu.make_async_copy(slot(k, i, other), x_v.at[other, pl.ds(i * piece, piece)], x_sem.at[other, i])
            for i in range(PIECES)
        ]

    def store_z(k, other):
        return [
            pltpu.make_async_copy(
                z_v.at[other, pl.ds(i * piece, piece)],
                z_ref.at[k, pl.ds(i * 2 * piece + other * piece, piece)],
                z_sem.at[other, i],
            )
            for i in range(PIECES)
        ]

    def compute(k, other):
        for i in range(PIECES):
            dev = source_of(me, k, i)
            dev = flip(dev, 1) if other else dev
            row = (labs_s[dev, pl.ds(i, 1), :] - me * columns).astype(F32)
            off_s[pl.ds(i * piece, piece), :] = as_column(row)[:piece].astype(jnp.int32)
        m_s[...] = jnp.full(m_s.shape, -jnp.inf, F32)
        s_s[...] = jnp.zeros(s_s.shape, F32)
        r_s[...] = jnp.zeros(r_s.shape, F32)

        @pl.when(k > 0)
        def _():
            wait(store_z(k, other))

        def body(j, carry):
            at = pl.multiple_of(j * wide, wide)
            z = dot(x_v[other], w_v[:, pl.ds(at, wide)], ((1,), (0,)))
            z_v[other, :, pl.ds(at, wide)] = z
            old = m_s[...]
            new = old
            for c in range(0, wide, 128):
                new = jnp.maximum(new, z[:, c : c + 128])
            total = s_s[...] * jnp.exp(old - new)
            right = r_s[...]
            off = off_s[...] - at
            for c in range(0, wide, 128):
                total += jnp.exp(z[:, c : c + 128] - new)
                right += jnp.where(lane == off - c, z[:, c : c + 128], 0.0)
            m_s[...] = new
            s_s[...] = total
            r_s[...] = right
            return carry

        lax.fori_loop(0, columns // wide, body, 0)
        start(store_z(k, other))
        high = jnp.max(m_s[...], -1, keepdims=True)
        total = jnp.sum(s_s[...] * jnp.exp(m_s[...] - high), -1, keepdims=True)
        right = jnp.sum(r_s[...], -1, keepdims=True)
        st_s[other] = jnp.where(lane == 0, high, jnp.where(lane == 1, total, jnp.where(lane == 2, right, 0.0)))

    def arrive(k):
        for i in range(PIECES):
            send(k, i).wait_recv()
        for later in range(1, BATCHES):
            if BEFORE[later] == k or (k == 1 and later == 4):
                start([send(later, i) for i in range(PIECES)])
        start([share(k, i) for i in range(PIECES)])
        start(load(k, 0))

    def load_shared(k):
        for i in range(PIECES):
            share(k, i).wait_recv()
        start(load(k, 1))

    load_shared(0)
    wait(w_copies)

    def batch(k, carry):
        compute(k, 0)

        @pl.when(k == 0)
        def _():
            wait(kept)

        for now in range(1, last):

            @pl.when(k + 1 == now)
            def _(now=now):
                arrive(now)

        @pl.when(k == last)
        def _():
            to_all(n, me, own_s, all_s, st_send, st_recv)
            load_shared(last)

        wait(load(k, 1))
        compute(k, 1)

        @pl.when(k + 1 == last)
        def _():
            arrive(last)

        @pl.when(k + 1 < last)
        def _():
            load_shared(k + 1)

        for i in range(PIECES):
            part = pl.ds(i * piece, piece)
            first, second = st_s[0, part, :], st_s[1, part, :]
            both = jnp.concatenate(
                [jnp.where(core == 0, first, second), jnp.where(core == 0, second, first)], 0
            ).T
            pair = lax.div(source_of(me, k, i), 2) * PIECES + i

            @pl.when(k < last)
            def _(i=i, both=both, pair=pair):
                for t in range(3):
                    own_s[t, pl.ds(pair, 1), :] = both[t : t + 1, :]

            @pl.when(k == last)
            def _(i=i, both=both):
                for t in range(3):
                    end_s[t, i : i + 1, :] = both[t : t + 1, :]

        @pl.when(k < last)
        def _():
            wait(load(k + 1, 0))

        return carry

    lax.fori_loop(0, BATCHES, batch, 0)

    all_s[me] = own_s[...]
    ends_s[me] = end_s[...]
    ends = to_all(n, me, end_s, ends_s, end_send, end_recv)
    stats = [all_copy(n, me, own_s, all_s, st_send, st_recv, j) for j in range(1, n)]
    for copy in stats + ends:
        copy.wait_recv()
    for dev in range(n):
        row = (n // 2 - 1 - dev // 2) * PIECES
        for t in range(3):
            all_s[dev, t, row : row + PIECES, :] = ends_s[dev, t, :PIECES, :]
    high, sums, right = all_s[:, 0], all_s[:, 1], all_s[:, 2]
    top = jnp.max(high, 0)
    total = jnp.sum(sums * jnp.exp(high - top[None]), 0)
    top_ref[...] = top
    inv_ref[...] = 1.0 / total
    loss_ref[...] = jnp.log(total) + top - jnp.sum(right, 0)
    for copy in labels + stats + ends:
        copy.wait_send()
    for k in range(BATCHES):
        for i in range(PIECES):
            share(k, i, k == 0).wait_send()
            if k > 0:
                send(k, i).wait_send()
    wait(store_z(last, 0) + store_z(last, 1))


def logits_call(n, x, w, lab):
    own, depth = x.shape
    columns = w.shape[1]
    pairs = n // 2 * PIECES
    anywhere, vmem = pl.BlockSpec(memory_space=pl.ANY), pl.BlockSpec(memory_space=pltpu.VMEM)
    dma = pltpu.SemaphoreType.DMA
    return pl.pallas_call(
        functools.partial(logits_kernel, n),
        in_specs=[anywhere, anywhere, vmem],
        out_specs=[anywhere, anywhere, vmem, vmem, vmem, vmem],
        out_shape=[
            jax.ShapeDtypeStruct((BATCHES, 2 * own, depth), BF16),
            jax.ShapeDtypeStruct((BATCHES, 2 * own, columns), F32),
            jax.ShapeDtypeStruct((pairs, 128), F32),
            jax.ShapeDtypeStruct((pairs, 128), F32),
            jax.ShapeDtypeStruct((pairs, 128), F32),
            jax.ShapeDtypeStruct((pairs, 128), F32),
        ],
        scratch_shapes=[
            pltpu.VMEM((depth, columns), BF16),
            pltpu.VMEM((2, own, depth), BF16),
            pltpu.VMEM((2, own, columns), F32),
            pltpu.VMEM((own, 128), F32),
            pltpu.VMEM((own, 128), F32),
            pltpu.VMEM((own, 128), F32),
            pltpu.VMEM((own, 128), jnp.int32),
            pltpu.VMEM((2, own, 128), F32),
            pltpu.VMEM((3, pairs, 128), F32),
            pltpu.VMEM((n, 3, pairs, 128), F32),
            pltpu.VMEM((3, 8, 128), F32),
            pltpu.VMEM((n, 3, 8, 128), F32),
            pltpu.VMEM((n,) + lab.shape, jnp.int32),
            dma((8,)),
            dma((2, PIECES)),
            dma((PIECES,)),
            dma((2, PIECES)),
            dma((BATCHES, PIECES)),
            dma((BATCHES, PIECES)),
            dma((BATCHES, PIECES)),
            dma((BATCHES, PIECES)),
            dma((n,)),
            dma((n,)),
            dma((n,)),
            dma((n,)),
            dma((n,)),
            dma((n,)),
        ],
        compiler_params=pltpu.CompilerParams(vmem_limit_bytes=VMEM_LIMIT, collective_id=0, has_side_effects=True),
        cost_estimate=pl.CostEstimate(flops=2 * n * own * depth * columns, bytes_accessed=1 << 27, transcendentals=0),
        name="gather_logits",
    )(x, w, lab)


PASSES = tuple((7 - t if t < 8 else None, 8 - t if t > 0 else None) for t in range(9))


def joins(k):
    return tuple(b for b in range(1, BATCHES) if BEFORE[b] == k)


def scatter_kernel(
    n, z_ref, w_ref, x_ref, top_ref, inv_ref, lab_ref,
    out_ref, g_ref, part_ref, took_ref, pass_ref, came_ref,
    z_v, g_v, w_v, in_v, p_v, o_v, last_v, fin_v, top_s, inv_s, off_s, gw_v,
    z_sem, g_sem, w_sem, in_sem, p_sem, o_sem, fin_sem, gw_sem, pair_recv, ici_send, ici_recv,
):
    me = lax.axis_index("tp")
    core = lax.rem(me, 2)
    half = z_ref.shape[1] // 2
    piece = half // PIECES
    depth, columns = w_ref.shape
    wide = w_v.shape[1]
    steps = depth // wide

    def start(copies):
        for copy in copies:
            copy.start()
        return copies

    def wait(copies):
        for copy in copies:
            copy.wait()

    def load_z(k, other, slot):
        return [
            pltpu.make_async_copy(
                z_ref.at[k, pl.ds(i * 2 * piece + other * piece, piece)],
                z_v.at[slot, pl.ds(i * piece, piece)],
                z_sem.at[slot, i],
            )
            for i in range(PIECES)
        ]

    def columns_at(j):
        return pl.ds(pl.multiple_of(j * wide, wide), wide)

    def load_w(j, slot):
        return pltpu.make_async_copy(w_ref.at[columns_at(j)], w_v.at[slot], w_sem.at[slot])

    def pass_on(k, i, like):
        part = pl.ds(i * piece, piece)
        return pltpu.make_async_remote_copy(
            src_ref=pass_ref.at[k, part],
            dst_ref=came_ref.at[k, part],
            send_sem=ici_send.at[k, i],
            recv_sem=ici_recv.at[k, i],
            device_id=across(me, i, like),
            device_id_type=MESH,
        )

    def load_g(k):
        to = pl.ds(pl.multiple_of(k * 2 * half, 2 * half), 2 * half)
        return [pltpu.make_async_copy(g_ref.at[k], gw_v.at[to], gw_sem.at[k])]

    start(load_z(7, 1, 0))
    load_w(0, 0).start()
    meet(n, me)

    lane = lax.broadcasted_iota(jnp.int32, (32, 128), 1)

    def run_pass(t, given, own, joined, like, after):
        final = t == len(PASSES) - 1 if isinstance(t, int) else False
        which = [(given, 1)] if own is None else [(own, 0)] if given is None else [(given, 1), (own, 0)]
        rows = half * len(which)
        g_copies = []
        for place, (k, other) in enumerate(which):
            slot = 0 if own is None else 1 - place
            for i in range(PIECES):
                pair = lax.div(source_of(me, jnp.int32(k), i), 2) * PIECES + i
                for from_ref, to_ref in ((top_ref, top_s), (inv_ref, inv_s), (lab_ref, off_s)):
                    both = as_column(from_ref[pl.ds(pair, 1), :])
                    to_ref[pl.ds(i * piece, piece), :] = jnp.where(core == other, both[:piece], both[piece:])
            wait(load_z(k, other, slot))
            if place + 1 < len(which):
                start(load_z(*which[1], 0))
            elif after is not None:
                start(load_z(*after, 1))

            def body(b, carry, slot=slot, place=place):
                part = pl.ds(pl.multiple_of(b * 32, 32), 32)
                to = pl.ds(pl.multiple_of(place * half + b * 32, 32), 32)
                top, inv, off = top_s[part, :], inv_s[part, :], off_s[part, :].astype(jnp.int32) - lane
                for c in range(0, columns, 128):
                    e = jnp.exp(z_v[slot, part, c : c + 128] - top) * inv
                    g_v[to, c : c + 128] = jnp.where(off == c, e - 1.0, e).astype(BF16)
                return carry

            lax.fori_loop(0, half // 32, body, 0)
            for i in range(PIECES):
                g_copies.append(
                    pltpu.make_async_copy(
                        g_v.at[pl.ds(place * half + i * piece, piece)],
                        g_ref.at[k, pl.ds(i * 2 * piece + other * piece, piece)],
                        g_sem.at[place, i],
                    )
                )
        start(g_copies)

        arrivals = []
        if own is not None:
            pltpu.make_async_remote_copy(
                src_ref=took_ref.at[own],
                dst_ref=took_ref.at[own],
                send_sem=p_sem.at[0],
                recv_sem=pair_recv.at[own],
                device_id={"tp": flip(me, 1)},
                device_id_type=MESH,
            ).wait_recv()
            arrivals.append(took_ref.at[own])
            for b in joined:
                for i in range(PIECES):
                    pass_on(b, i, b).wait_recv()
                arrivals.append(came_ref.at[b])

        def load_in(j, slot):
            return [
                pltpu.make_async_copy(ref.at[:, columns_at(j)], in_v.at[slot, m], in_sem.at[slot, m])
                for m, ref in enumerate(arrivals)
            ]

        def outs(j, slot):
            copies = []
            if given is not None:
                copies.append(
                    pltpu.make_async_remote_copy(
                        src_ref=p_v.at[slot],
                        dst_ref=took_ref.at[given, :, columns_at(j)],
                        send_sem=p_sem.at[slot],
                        recv_sem=pair_recv.at[given],
                        device_id={"tp": flip(me, 1)},
                        device_id_type=MESH,
                    )
                )
            if own is not None and not final:
                copies.append(pltpu.make_async_copy(o_v.at[slot], pass_ref.at[own, :, columns_at(j)], o_sem.at[slot]))
            return copies

        def finished(copies):
            for m, copy in enumerate(copies):
                if m == 0 and given is not None:
                    copy.wait_send()
                else:
                    copy.wait()

        def slot_at(j):
            return lax.rem(jnp.int32(t) * steps + j, 2)

        start(load_in(0, slot_at(0)))

        def multiply(j, carry):
            slot = slot_at(j)
            if not final:
                load_w(lax.rem(j + 1, steps), 1 - slot).start()

            @pl.when(j + 1 < steps)
            def _():
                if final:
                    load_w(j + 1, 1 - slot).start()
                start(load_in(j + 1, 1 - slot))

            @pl.when(j > 0)
            def _():
                start(outs(j - 1, 1 - slot))

            @pl.when(j > 1)
            def _():
                finished(outs(j - 2, slot))

            load_w(j, slot).wait()
            wait(load_in(j, slot))
            term = dot(g_v[:rows, :], w_v[slot], ((1,), (1,)))
            if given is not None:
                p_v[slot] = term[:half].astype(BF16)
            if own is not None:
                value = term[rows - half :]
                for m in range(len(arrivals)):
                    value = value + in_v[slot, m].astype(F32)
                if final:
                    last_v[:, columns_at(j)] = value
                else:
                    o_v[slot] = value.astype(BF16)
            return carry

        lax.fori_loop(0, steps, multiply, 0)
        start(outs(steps - 1, slot_at(steps - 1)))
        for j in (steps - 2, steps - 1):
            finished(outs(j, slot_at(j)))
        wait(g_copies)
        if own is not None:
            if not final:
                start([pass_on(own, i, like) for i in range(PIECES)])
            start(load_g(own))

    run_pass(0, 7, None, (), None, (6, 1))

    def plain(t, carry):
        run_pass(t, 7 - t, 8 - t, (), 4, (6 - t, 1))
        return carry

    lax.fori_loop(1, 5, plain, 0)
    for t in range(5, len(PASSES)):
        given, own = PASSES[t]
        after = None if given is None else (given - 1, 1) if given > 0 else (0, 0)
        run_pass(t, given, own, joins(own) if own else (), own if own else None, after)

    for k in range(BATCHES):
        wait(load_g(k))
    ends = []
    for m, b in enumerate((4, 2)):
        for i in range(PIECES):
            pass_on(b, i, b).wait_recv()
        ends += start([pltpu.make_async_copy(came_ref.at[b], fin_v.at[m], fin_sem.at[m])])

    def outer(x_tile, out_tile):
        out_tile[...] = dot(x_tile[...], gw_v[...], ((0,), (0,))).astype(BF16)

    pltpu.emit_pipeline(
        outer,
        grid=(part_ref.shape[0] // BY_W_TALL,),
        in_specs=[pl.BlockSpec((BATCHES * 2 * half, BY_W_TALL), lambda j: (0, j))],
        out_specs=[pl.BlockSpec((BY_W_TALL, columns), lambda j: (j, 0))],
    )(x_ref, part_ref)

    for i in range(PIECES):
        pass_on(1, i, 1).wait_recv()
    ends += start([pltpu.make_async_copy(came_ref.at[1], fin_v.at[2], fin_sem.at[2])])
    wait(ends)

    def finish(j, carry):
        at = columns_at(j)
        value = last_v[:, at]
        for m in range(len(joins(0))):
            value = value + fin_v[m, :, at].astype(F32)
        fin_v[0, :, at] = value.astype(BF16)
        return carry

    lax.fori_loop(0, steps, finish, 0)
    wait(start([pltpu.make_async_copy(fin_v.at[0], out_ref, fin_sem.at[0])]))
    for k in range(1, BATCHES):
        for i in range(PIECES):
            pass_on(k, i, k).wait_send()


def scatter_call(n, z, w, xb, top, inv, lab):
    depth, columns = w.shape
    half, wide = z.shape[1] // 2, 2048
    anywhere, vmem = pl.BlockSpec(memory_space=pl.ANY), pl.BlockSpec(memory_space=pltpu.VMEM)
    dma = pltpu.SemaphoreType.DMA
    moved = jax.ShapeDtypeStruct((BATCHES, half, depth), BF16)
    most = 1 + max(len(joins(k)) for k in range(1, BATCHES))
    return pl.pallas_call(
        functools.partial(scatter_kernel, n),
        in_specs=[anywhere, anywhere, anywhere, vmem, vmem, vmem],
        out_specs=[anywhere] * 6,
        out_shape=[
            jax.ShapeDtypeStruct((half, depth), BF16),
            jax.ShapeDtypeStruct(z.shape, BF16),
            jax.ShapeDtypeStruct((BY_W_EARLY * BY_W_TALL, columns), BF16),
            moved,
            moved,
            moved,
        ],
        scratch_shapes=[
            pltpu.VMEM((2, half, columns), F32),
            pltpu.VMEM((2 * half, columns), BF16),
            pltpu.VMEM((2, wide, columns), BF16),
            pltpu.VMEM((2, most, half, wide), BF16),
            pltpu.VMEM((2, half, wide), BF16),
            pltpu.VMEM((2, half, wide), BF16),
            pltpu.VMEM((half, depth), F32),
            pltpu.VMEM((len(joins(0)), half, depth), BF16),
            pltpu.VMEM((half, 128), F32),
            pltpu.VMEM((half, 128), F32),
            pltpu.VMEM((half, 128), F32),
            pltpu.VMEM((BATCHES * 2 * half, columns), BF16),
            dma((2, PIECES)),
            dma((2, PIECES)),
            dma((2,)),
            dma((2, most)),
            dma((2,)),
            dma((2,)),
            dma((3,)),
            dma((BATCHES,)),
            dma((BATCHES,)),
            dma((BATCHES, PIECES)),
            dma((BATCHES, PIECES)),
        ],
        compiler_params=pltpu.CompilerParams(vmem_limit_bytes=VMEM_LIMIT, collective_id=1, has_side_effects=True),
        cost_estimate=pl.CostEstimate(flops=3 * n * half * depth * columns, bytes_accessed=1 << 28, transcendentals=0),
        name="by_x_scatter",
    )(z, w, xb, top, inv, lab)


def by_w_kernel(x_ref, g_ref, part_ref, by_x_ref, out_ref, by_x_out_ref, g_v, part_v, by_x_v, g_sem, part_sem):
    rows, columns = g_ref.shape
    early = part_ref.shape[0]
    g_load = [
        pltpu.make_async_copy(g_ref.at[pl.ds(p * rows // 8, rows // 8)], g_v.at[pl.ds(p * rows // 8, rows // 8)], g_sem.at[p])
        for p in range(8)
    ]
    load = pltpu.make_async_copy(part_ref, part_v, part_sem.at[0])
    for copy in g_load:
        copy.start()
    by_x_load = pltpu.make_async_copy(by_x_ref, by_x_v, part_sem.at[2])
    for copy in g_load:
        copy.wait()
    load.start()
    by_x_load.start()

    def outer(x_tile, out_tile):
        out_tile[...] = dot(x_tile[...], g_v[...], ((0,), (0,))).astype(BF16)

    tiles = (out_ref.shape[0] - early) // BY_W_TALL

    def run(first, count):
        skip = early // BY_W_TALL + first
        pltpu.emit_pipeline(
            outer,
            grid=(count,),
            in_specs=[pl.BlockSpec((rows, BY_W_TALL), lambda j: (0, skip + j))],
            out_specs=[pl.BlockSpec((BY_W_TALL, columns), lambda j: (skip + j, 0))],
        )(x_ref, out_ref)

    run(0, tiles // 2)
    load.wait()
    store = pltpu.make_async_copy(part_v, out_ref.at[pl.ds(0, early)], part_sem.at[1])
    store.start()
    by_x_load.wait()
    by_x_store = pltpu.make_async_copy(by_x_v, by_x_out_ref, part_sem.at[3])
    by_x_store.start()
    run(tiles // 2, tiles - tiles // 2)
    store.wait()
    by_x_store.wait()


def by_w_call(xb, g, part, by_x):
    rows, depth = xb.shape
    columns = g.shape[1]
    anywhere = pl.BlockSpec(memory_space=pl.ANY)
    dma = pltpu.SemaphoreType.DMA
    return pl.pallas_call(
        by_w_kernel,
        in_specs=[anywhere] * 4,
        out_specs=[anywhere] * 2,
        out_shape=[jax.ShapeDtypeStruct((depth, columns), BF16), jax.ShapeDtypeStruct(by_x.shape, BF16)],
        scratch_shapes=[
            pltpu.VMEM((rows, columns), BF16),
            pltpu.VMEM(part.shape, BF16),
            pltpu.VMEM(by_x.shape, BF16),
            dma((8,)),
            dma((4,)),
        ],
        compiler_params=pltpu.CompilerParams(vmem_limit_bytes=VMEM_LIMIT),
        cost_estimate=pl.CostEstimate(flops=rows * depth * columns, bytes_accessed=1 << 26, transcendentals=0),
        name="by_w",
    )(xb, g, part, by_x)


def solution(mesh):
    n = mesh.shape["tp"]

    def step(x, w, label):
        me, own, columns = lax.axis_index("tp"), x.shape[0], w.shape[1]
        piece = own // PIECES
        lab = jnp.pad(label.reshape(PIECES, piece), ((0, 0), (0, 128 - piece)))
        xb, z, rel, top, inv, loss = logits_call(n, x, w, lab)
        by_x, g, part, *_ = scatter_call(n, z, w, xb.reshape(-1, xb.shape[-1]), top, inv, rel)
        by_w, by_x = by_w_call(xb.reshape(-1, xb.shape[-1]), g.reshape(-1, columns), part, by_x)
        by_device = loss.reshape(n // 2, PIECES, 2, piece).swapaxes(1, 2).reshape(n, own)
        return lax.dynamic_index_in_dim(by_device, me, 0, keepdims=False), by_x, by_w

    return jax.shard_map(
        step,
        mesh=mesh,
        in_specs=(P(("dp", "tp"), None), P(None, "tp"), P(("dp", "tp"))),
        out_specs=(P(("dp", "tp")), P(("dp", "tp"), None), P("dp", "tp")),
        check_vma=False,
    )
```

```python
import functools

import jax
import jax.numpy as jnp
from jax import lax
from jax.experimental import pallas as pl
from jax.experimental.pallas import tpu as pltpu
from jax.sharding import PartitionSpec as P

F32, BF16 = jnp.float32, jnp.bfloat16
MESH = pl.DeviceIdType.MESH
VMEM_LIMIT = 63 * 1024 * 1024

ORDERS = ((4, 2, 1), (2, 1, 4), (1, 4, 2))
LAST = (None, 0, 1, 1, 2, 2, 2, 2)
BEFORE = (None, 0, 0, 1, 0, 1, 2, 3)
BATCHES, PIECES = 8, 3
BY_W_TALL = 256
BY_W_EARLY = 10


def dot(a, b, contract):
    return lax.dot_general(a, b, (contract, ((), ())), preferred_element_type=F32)


def flip(index, mask):
    for bit in (1, 2, 4, 8):
        if mask & bit:
            index = index + bit - 2 * bit * lax.rem(lax.div(index, bit), 2)
    return index


def source_of(me, k, i):
    index = me
    for bit, on in zip(ORDERS[i], (lax.rem(k, 2), lax.rem(lax.div(k, 2), 2), lax.div(k, 4))):
        index = index + on * (2 * bit) * (1 - 2 * lax.rem(lax.div(me, 2 * bit), 2))
    return index


def across(me, i, k):
    return {"tp": flip(me, 2 * ORDERS[i][LAST[k]])}


def meet(n, me):
    barrier = pltpu.get_barrier_semaphore()
    for j in range(1, n):
        pl.semaphore_signal(barrier, inc=1, device_id={"tp": lax.rem(me + j, n)}, device_id_type=MESH)
    pl.semaphore_wait(barrier, n - 1)


def all_copy(n, me, own_ref, all_ref, send_sems, recv_sems, j):
    return pltpu.make_async_remote_copy(
        src_ref=own_ref,
        dst_ref=all_ref.at[me],
        send_sem=send_sems.at[j],
        recv_sem=recv_sems.at[j],
        device_id={"tp": lax.rem(me + j, n)},
        device_id_type=MESH,
    )


def to_all(n, me, own_ref, all_ref, send_sems, recv_sems):
    copies = [all_copy(n, me, own_ref, all_ref, send_sems, recv_sems, j) for j in range(1, n)]
    for copy in copies:
        copy.start()
    return copies


def as_column(row):
    return jnp.broadcast_to(row, (128, 128)).T


def logits_kernel(
    n, x_ref, w_ref, lab_ref, xb_ref, z_ref, rel_ref, top_ref, inv_ref, loss_ref,
    w_v, x_v, z_v, m_s, s_s, r_s, off_s, st_s, own_s, all_s, end_s, ends_s, labs_s,
    w_sem, x_sem, keep_sem, z_sem, ici_send, ici_recv, pair_send, pair_recv, lab_send, lab_recv, st_send, st_recv,
    end_send, end_recv,
):
    me = lax.axis_index("tp")
    core = lax.rem(me, 2)
    piece = x_ref.shape[0] // PIECES
    half = PIECES * piece
    depth, columns = w_ref.shape
    wide = 1024
    last = BATCHES - 1

    def start(copies):
        for copy in copies:
            copy.start()
        return copies

    def wait(copies):
        for copy in copies:
            copy.wait()

    w_parts = 8
    w_copies = []
    for p in range(w_parts):
        part = pl.ds(p * (depth // w_parts), depth // w_parts)
        w_copies.append(pltpu.make_async_copy(w_ref.at[part], w_v.at[part], w_sem.at[p]))
    x_load = pltpu.make_async_copy(x_ref, x_v.at[0], x_sem.at[0, 0])
    start([x_load] + w_copies)
    own_s[...] = jnp.zeros(own_s.shape, F32)
    end_s[...] = jnp.zeros(end_s.shape, F32)

    meet(n, me)

    def slot(k, i, other):
        return xb_ref.at[k, pl.ds(i * 2 * piece + other * piece, piece)]

    def source(k, i):
        return x_ref.at[pl.ds(i * piece, piece)] if k == 0 else slot(k, i, 0)

    def send(k, i):
        return pltpu.make_async_remote_copy(
            src_ref=source(BEFORE[k], i),
            dst_ref=slot(k, i, 0),
            send_sem=ici_send.at[k, i],
            recv_sem=ici_recv.at[k, i],
            device_id=across(me, i, k),
            device_id_type=MESH,
        )

    def share(k, i, from_x=False):
        return pltpu.make_async_remote_copy(
            src_ref=source(0, i) if from_x else slot(k, i, 0),
            dst_ref=slot(k, i, 1),
            send_sem=pair_send.at[k, i],
            recv_sem=pair_recv.at[k, i],
            device_id={"tp": flip(me, 1)},
            device_id_type=MESH,
        )

    labels = to_all(n, me, lab_ref, labs_s, lab_send, lab_recv)
    start([send(1, i) for i in range(PIECES)])
    start([share(0, i, True) for i in range(PIECES)])
    start([send(2, i) for i in range(PIECES)])
    labs_s[me] = lab_ref[...]
    x_load.wait()
    kept = start(
        [pltpu.make_async_copy(x_v.at[0, pl.ds(i * piece, piece)], slot(0, i, 0), keep_sem.at[i]) for i in range(PIECES)]
    )
    for copy in labels:
        copy.wait_recv()
    low = lax.broadcasted_iota(jnp.int32, (1, 128), 1) < piece
    for chip in range(n // 2):
        for i in range(PIECES):
            first, second = labs_s[2 * chip, i : i + 1, :].astype(F32), labs_s[2 * chip + 1, i : i + 1, :].astype(F32)
            rel_ref[chip * PIECES + i : chip * PIECES + i + 1, :] = (
                jnp.where(low, first, pltpu.roll(second, piece, 1)) - (me * columns).astype(F32)
            )

    lane = lax.broadcasted_iota(jnp.int32, (half, 128), 1)

    def load(k, other):
        return [
            pltpu.make_async_copy(slot(k, i, other), x_v.at[other, pl.ds(i * piece, piece)], x_sem.at[other, i])
            for i in range(PIECES)
        ]

    def store_z(k, other):
        return [
            pltpu.make_async_copy(
                z_v.at[other, pl.ds(i * piece, piece)],
                z_ref.at[k, pl.ds(i * 2 * piece + other * piece, piece)],
                z_sem.at[other, i],
            )
            for i in range(PIECES)
        ]

    def compute(k, other):
        for i in range(PIECES):
            dev = source_of(me, k, i)
            dev = flip(dev, 1) if other else dev
            row = (labs_s[dev, pl.ds(i, 1), :] - me * columns).astype(F32)
            off_s[pl.ds(i * piece, piece), :] = as_column(row)[:piece].astype(jnp.int32)
        m_s[...] = jnp.full(m_s.shape, -jnp.inf, F32)
        s_s[...] = jnp.zeros(s_s.shape, F32)
        r_s[...] = jnp.zeros(r_s.shape, F32)

        @pl.when(k > 0)
        def _():
            wait(store_z(k, other))

        def body(j, carry):
            at = pl.multiple_of(j * wide, wide)
            z = dot(x_v[other], w_v[:, pl.ds(at, wide)], ((1,), (0,)))
            z_v[other, :, pl.ds(at, wide)] = z
            old = m_s[...]
            new = old
            for c in range(0, wide, 128):
                new = jnp.maximum(new, z[:, c : c + 128])
            total = s_s[...] * jnp.exp(old - new)
            right = r_s[...]
            off = off_s[...] - at
            for c in range(0, wide, 128):
                total += jnp.exp(z[:, c : c + 128] - new)
                right += jnp.where(lane == off - c, z[:, c : c + 128], 0.0)
            m_s[...] = new
            s_s[...] = total
            r_s[...] = right
            return carry

        lax.fori_loop(0, columns // wide, body, 0)
        start(store_z(k, other))
        high = jnp.max(m_s[...], -1, keepdims=True)
        total = jnp.sum(s_s[...] * jnp.exp(m_s[...] - high), -1, keepdims=True)
        right = jnp.sum(r_s[...], -1, keepdims=True)
        st_s[other] = jnp.where(lane == 0, high, jnp.where(lane == 1, total, jnp.where(lane == 2, right, 0.0)))

    def arrive(k):
        for i in range(PIECES):
            send(k, i).wait_recv()
        for later in range(1, BATCHES):
            if BEFORE[later] == k or (k == 1 and later == 4):
                start([send(later, i) for i in range(PIECES)])
        start([share(k, i) for i in range(PIECES)])
        start(load(k, 0))

    def load_shared(k):
        for i in range(PIECES):
            share(k, i).wait_recv()
        start(load(k, 1))

    load_shared(0)
    wait(w_copies)

    def batch(k, carry):
        compute(k, 0)

        @pl.when(k == 0)
        def _():
            wait(kept)

        for now in range(1, last):

            @pl.when(k + 1 == now)
            def _(now=now):
                arrive(now)

        @pl.when(k == last)
        def _():
            to_all(n, me, own_s, all_s, st_send, st_recv)
            load_shared(last)

        wait(load(k, 1))
        compute(k, 1)

        @pl.when(k + 1 == last)
        def _():
            arrive(last)

        @pl.when(k + 1 < last)
        def _():
            load_shared(k + 1)

        for i in range(PIECES):
            part = pl.ds(i * piece, piece)
            first, second = st_s[0, part, :], st_s[1, part, :]
            both = jnp.concatenate(
                [jnp.where(core == 0, first, second), jnp.where(core == 0, second, first)], 0
            ).T
            pair = lax.div(source_of(me, k, i), 2) * PIECES + i

            @pl.when(k < last)
            def _(i=i, both=both, pair=pair):
                for t in range(3):
                    own_s[t, pl.ds(pair, 1), :] = both[t : t + 1, :]

            @pl.when(k == last)
            def _(i=i, both=both):
                for t in range(3):
                    end_s[t, i : i + 1, :] = both[t : t + 1, :]

        @pl.when(k < last)
        def _():
            wait(load(k + 1, 0))

        return carry

    lax.fori_loop(0, BATCHES, batch, 0)

    all_s[me] = own_s[...]
    ends_s[me] = end_s[...]
    ends = to_all(n, me, end_s, ends_s, end_send, end_recv)
    stats = [all_copy(n, me, own_s, all_s, st_send, st_recv, j) for j in range(1, n)]
    for copy in stats + ends:
        copy.wait_recv()
    for dev in range(n):
        row = (n // 2 - 1 - dev // 2) * PIECES
        for t in range(3):
            all_s[dev, t, row : row + PIECES, :] = ends_s[dev, t, :PIECES, :]
    high, sums, right = all_s[:, 0], all_s[:, 1], all_s[:, 2]
    top = jnp.max(high, 0)
    total = jnp.sum(sums * jnp.exp(high - top[None]), 0)
    top_ref[...] = top
    inv_ref[...] = 1.0 / total
    loss_ref[...] = jnp.log(total) + top - jnp.sum(right, 0)
    for copy in labels + stats + ends:
        copy.wait_send()
    for k in range(BATCHES):
        for i in range(PIECES):
            share(k, i, k == 0).wait_send()
            if k > 0:
                send(k, i).wait_send()
    wait(store_z(last, 0) + store_z(last, 1))


def logits_call(n, x, w, lab):
    own, depth = x.shape
    columns = w.shape[1]
    pairs = n // 2 * PIECES
    anywhere, vmem = pl.BlockSpec(memory_space=pl.ANY), pl.BlockSpec(memory_space=pltpu.VMEM)
    dma = pltpu.SemaphoreType.DMA
    return pl.pallas_call(
        functools.partial(logits_kernel, n),
        in_specs=[anywhere, anywhere, vmem],
        out_specs=[anywhere, anywhere, vmem, vmem, vmem, vmem],
        out_shape=[
            jax.ShapeDtypeStruct((BATCHES, 2 * own, depth), BF16),
            jax.ShapeDtypeStruct((BATCHES, 2 * own, columns), F32),
            jax.ShapeDtypeStruct((pairs, 128), F32),
            jax.ShapeDtypeStruct((pairs, 128), F32),
            jax.ShapeDtypeStruct((pairs, 128), F32),
            jax.ShapeDtypeStruct((pairs, 128), F32),
        ],
        scratch_shapes=[
            pltpu.VMEM((depth, columns), BF16),
            pltpu.VMEM((2, own, depth), BF16),
            pltpu.VMEM((2, own, columns), F32),
            pltpu.VMEM((own, 128), F32),
            pltpu.VMEM((own, 128), F32),
            pltpu.VMEM((own, 128), F32),
            pltpu.VMEM((own, 128), jnp.int32),
            pltpu.VMEM((2, own, 128), F32),
            pltpu.VMEM((3, pairs, 128), F32),
            pltpu.VMEM((n, 3, pairs, 128), F32),
            pltpu.VMEM((3, 8, 128), F32),
            pltpu.VMEM((n, 3, 8, 128), F32),
            pltpu.VMEM((n,) + lab.shape, jnp.int32),
            dma((8,)),
            dma((2, PIECES)),
            dma((PIECES,)),
            dma((2, PIECES)),
            dma((BATCHES, PIECES)),
            dma((BATCHES, PIECES)),
            dma((BATCHES, PIECES)),
            dma((BATCHES, PIECES)),
            dma((n,)),
            dma((n,)),
            dma((n,)),
            dma((n,)),
            dma((n,)),
            dma((n,)),
        ],
        compiler_params=pltpu.CompilerParams(vmem_limit_bytes=VMEM_LIMIT, collective_id=0, has_side_effects=True),
        cost_estimate=pl.CostEstimate(flops=2 * n * own * depth * columns, bytes_accessed=1 << 27, transcendentals=0),
        name="gather_logits",
    )(x, w, lab)


PASSES = tuple((7 - t if t < 8 else None, 8 - t if t > 0 else None) for t in range(9))


def joins(k):
    return tuple(b for b in range(1, BATCHES) if BEFORE[b] == k)


def scatter_kernel(
    n, z_ref, w_ref, x_ref, top_ref, inv_ref, lab_ref,
    out_ref, g_ref, part_ref, took_ref, pass_ref, came_ref,
    z_v, g_v, w_v, in_v, p_v, o_v, last_v, fin_v, top_s, inv_s, off_s, gw_v,
    z_sem, g_sem, w_sem, in_sem, p_sem, o_sem, fin_sem, gw_sem, pair_recv, ici_send, ici_recv,
):
    me = lax.axis_index("tp")
    core = lax.rem(me, 2)
    half = z_ref.shape[1] // 2
    piece = half // PIECES
    depth, columns = w_ref.shape
    wide = w_v.shape[1]
    steps = depth // wide

    def start(copies):
        for copy in copies:
            copy.start()
        return copies

    def wait(copies):
        for copy in copies:
            copy.wait()

    def load_z(k, other, slot):
        return [
            pltpu.make_async_copy(
                z_ref.at[k, pl.ds(i * 2 * piece + other * piece, piece)],
                z_v.at[slot, pl.ds(i * piece, piece)],
                z_sem.at[slot, i],
            )
            for i in range(PIECES)
        ]

    def columns_at(j):
        return pl.ds(pl.multiple_of(j * wide, wide), wide)

    def load_w(j, slot):
        return pltpu.make_async_copy(w_ref.at[columns_at(j)], w_v.at[slot], w_sem.at[slot])

    def pass_on(k, i, like):
        part = pl.ds(i * piece, piece)
        return pltpu.make_async_remote_copy(
            src_ref=pass_ref.at[k, part],
            dst_ref=came_ref.at[k, part],
            send_sem=ici_send.at[k, i],
            recv_sem=ici_recv.at[k, i],
            device_id=across(me, i, like),
            device_id_type=MESH,
        )

    def load_g(k):
        to = pl.ds(pl.multiple_of(k * 2 * half, 2 * half), 2 * half)
        return [pltpu.make_async_copy(g_ref.at[k], gw_v.at[to], gw_sem.at[k])]

    start(load_z(7, 1, 0))
    load_w(0, 0).start()
    meet(n, me)

    lane = lax.broadcasted_iota(jnp.int32, (32, 128), 1)

    def run_pass(t, given, own, joined, like, after):
        final = t == len(PASSES) - 1 if isinstance(t, int) else False
        which = [(given, 1)] if own is None else [(own, 0)] if given is None else [(given, 1), (own, 0)]
        rows = half * len(which)
        g_copies = []
        arrivals = [] if own is None else [took_ref.at[own]] + [came_ref.at[b] for b in joined]

        def load_in(j, slot):
            return [
                pltpu.make_async_copy(ref.at[:, columns_at(j)], in_v.at[slot, m], in_sem.at[slot, m])
                for m, ref in enumerate(arrivals)
            ]

        def slot_at(j):
            return lax.rem(jnp.int32(t) * steps + j, 2)

        def take_in():
            if own is None:
                return
            partner = pltpu.make_async_remote_copy(
                src_ref=took_ref.at[own],
                dst_ref=took_ref.at[own],
                send_sem=p_sem.at[0],
                recv_sem=pair_recv.at[own],
                device_id={"tp": flip(me, 1)},
                device_id_type=MESH,
            )
            partner.wait_recv()
            for b in joined:
                for i in range(PIECES):
                    pass_on(b, i, b).wait_recv()
            start(load_in(0, slot_at(0)))
            before = lax.rem(jnp.int32(t) * steps + 1, 2)
            pltpu.make_async_remote_copy(
                src_ref=p_v.at[before],
                dst_ref=took_ref.at[own, :, columns_at(0)],
                send_sem=p_sem.at[before],
                recv_sem=pair_recv.at[own],
                device_id={"tp": flip(me, 1)},
                device_id_type=MESH,
            ).wait_send()

        for place, (k, other) in enumerate(which):
            slot = 0 if own is None else 1 - place
            for i in range(PIECES):
                pair = lax.div(source_of(me, jnp.int32(k), i), 2) * PIECES + i
                for from_ref, to_ref in ((top_ref, top_s), (inv_ref, inv_s), (lab_ref, off_s)):
                    both = as_column(from_ref[pl.ds(pair, 1), :])
                    to_ref[pl.ds(i * piece, piece), :] = jnp.where(core == other, both[:piece], both[piece:])
            wait(load_z(k, other, slot))
            if place + 1 < len(which):
                start(load_z(*which[1], 0))
            elif after is not None:
                start(load_z(*after, 1))

            def body(b, carry, slot=slot, place=place):
                part = pl.ds(pl.multiple_of(b * 32, 32), 32)
                to = pl.ds(pl.multiple_of(place * half + b * 32, 32), 32)
                top, inv, off = top_s[part, :], inv_s[part, :], off_s[part, :].astype(jnp.int32) - lane
                for c in range(0, columns, 128):
                    e = jnp.exp(z_v[slot, part, c : c + 128] - top) * inv
                    g_v[to, c : c + 128] = jnp.where(off == c, e - 1.0, e).astype(BF16)
                return carry

            lax.fori_loop(0, half // 32, body, 0)
            if place == 0:
                take_in()
            for i in range(PIECES):
                g_copies.append(
                    pltpu.make_async_copy(
                        g_v.at[pl.ds(place * half + i * piece, piece)],
                        g_ref.at[k, pl.ds(i * 2 * piece + other * piece, piece)],
                        g_sem.at[place, i],
                    )
                )
        start(g_copies)

        def outs(j, slot):
            copies = []
            if given is not None:
                copies.append(
                    pltpu.make_async_remote_copy(
                        src_ref=p_v.at[slot],
                        dst_ref=took_ref.at[given, :, columns_at(j)],
                        send_sem=p_sem.at[slot],
                        recv_sem=pair_recv.at[given],
                        device_id={"tp": flip(me, 1)},
                        device_id_type=MESH,
                    )
                )
            if own is not None and not final:
                copies.append(pltpu.make_async_copy(o_v.at[slot], pass_ref.at[own, :, columns_at(j)], o_sem.at[slot]))
            return copies

        def finished(copies):
            for m, copy in enumerate(copies):
                if m == 0 and given is not None:
                    copy.wait_send()
                else:
                    copy.wait()

        def multiply(j, carry):
            slot = slot_at(j)
            if not final:
                load_w(lax.rem(j + 1, steps), 1 - slot).start()

            @pl.when(j + 1 < steps)
            def _():
                if final:
                    load_w(j + 1, 1 - slot).start()
                start(load_in(j + 1, 1 - slot))

            @pl.when(j > 0)
            def _():
                start(outs(j - 1, 1 - slot))

            @pl.when(j > 1)
            def _():
                finished(outs(j - 2, slot))

            load_w(j, slot).wait()
            wait(load_in(j, slot))
            term = dot(g_v[:rows, :], w_v[slot], ((1,), (1,)))
            if given is not None:
                p_v[slot] = term[:half].astype(BF16)
            if own is not None:
                value = term[rows - half :]
                for m in range(len(arrivals)):
                    value = value + in_v[slot, m].astype(F32)
                if final:
                    last_v[:, columns_at(j)] = value
                else:
                    o_v[slot] = value.astype(BF16)
            return carry

        lax.fori_loop(0, steps, multiply, 0)
        ending = start(outs(steps - 1, slot_at(steps - 1)))
        finished(outs(steps - 2, slot_at(steps - 2)))
        wait(ending if given is None else ending[1:])
        wait(g_copies)
        if own is not None:
            if not final:
                start([pass_on(own, i, like) for i in range(PIECES)])
            start(load_g(own))

    run_pass(0, 7, None, (), None, (6, 1))

    def plain(t, carry):
        run_pass(t, 7 - t, 8 - t, (), 4, (6 - t, 1))
        return carry

    lax.fori_loop(1, 5, plain, 0)
    for t in range(5, len(PASSES)):
        given, own = PASSES[t]
        after = None if given is None else (given - 1, 1) if given > 0 else (0, 0)
        run_pass(t, given, own, joins(own) if own else (), own if own else None, after)

    for k in range(BATCHES):
        wait(load_g(k))
    ends = []
    for m, b in enumerate((4, 2)):
        for i in range(PIECES):
            pass_on(b, i, b).wait_recv()
        ends += start([pltpu.make_async_copy(came_ref.at[b], fin_v.at[m], fin_sem.at[m])])

    def outer(x_tile, out_tile):
        out_tile[...] = dot(x_tile[...], gw_v[...], ((0,), (0,))).astype(BF16)

    pltpu.emit_pipeline(
        outer,
        grid=(part_ref.shape[0] // BY_W_TALL,),
        in_specs=[pl.BlockSpec((BATCHES * 2 * half, BY_W_TALL), lambda j: (0, j))],
        out_specs=[pl.BlockSpec((BY_W_TALL, columns), lambda j: (j, 0))],
    )(x_ref, part_ref)

    for i in range(PIECES):
        pass_on(1, i, 1).wait_recv()
    ends += start([pltpu.make_async_copy(came_ref.at[1], fin_v.at[2], fin_sem.at[2])])
    wait(ends)

    def finish(j, carry):
        at = columns_at(j)
        value = last_v[:, at]
        for m in range(len(joins(0))):
            value = value + fin_v[m, :, at].astype(F32)
        fin_v[0, :, at] = value.astype(BF16)
        return carry

    lax.fori_loop(0, steps, finish, 0)
    wait(start([pltpu.make_async_copy(fin_v.at[0], out_ref, fin_sem.at[0])]))
    for k in range(1, BATCHES):
        for i in range(PIECES):
            pass_on(k, i, k).wait_send()


def scatter_call(n, z, w, xb, top, inv, lab):
    depth, columns = w.shape
    half, wide = z.shape[1] // 2, 2048
    anywhere, vmem = pl.BlockSpec(memory_space=pl.ANY), pl.BlockSpec(memory_space=pltpu.VMEM)
    dma = pltpu.SemaphoreType.DMA
    moved = jax.ShapeDtypeStruct((BATCHES, half, depth), BF16)
    most = 1 + max(len(joins(k)) for k in range(1, BATCHES))
    return pl.pallas_call(
        functools.partial(scatter_kernel, n),
        in_specs=[anywhere, anywhere, anywhere, vmem, vmem, vmem],
        out_specs=[anywhere] * 6,
        out_shape=[
            jax.ShapeDtypeStruct((half, depth), BF16),
            jax.ShapeDtypeStruct(z.shape, BF16),
            jax.ShapeDtypeStruct((BY_W_EARLY * BY_W_TALL, columns), BF16),
            moved,
            moved,
            moved,
        ],
        scratch_shapes=[
            pltpu.VMEM((2, half, columns), F32),
            pltpu.VMEM((2 * half, columns), BF16),
            pltpu.VMEM((2, wide, columns), BF16),
            pltpu.VMEM((2, most, half, wide), BF16),
            pltpu.VMEM((2, half, wide), BF16),
            pltpu.VMEM((2, half, wide), BF16),
            pltpu.VMEM((half, depth), F32),
            pltpu.VMEM((len(joins(0)), half, depth), BF16),
            pltpu.VMEM((half, 128), F32),
            pltpu.VMEM((half, 128), F32),
            pltpu.VMEM((half, 128), F32),
            pltpu.VMEM((BATCHES * 2 * half, columns), BF16),
            dma((2, PIECES)),
            dma((2, PIECES)),
            dma((2,)),
            dma((2, most)),
            dma((2,)),
            dma((2,)),
            dma((3,)),
            dma((BATCHES,)),
            dma((BATCHES,)),
            dma((BATCHES, PIECES)),
            dma((BATCHES, PIECES)),
        ],
        compiler_params=pltpu.CompilerParams(vmem_limit_bytes=VMEM_LIMIT, collective_id=1, has_side_effects=True),
        cost_estimate=pl.CostEstimate(flops=3 * n * half * depth * columns, bytes_accessed=1 << 28, transcendentals=0),
        name="by_x_scatter",
    )(z, w, xb, top, inv, lab)


def by_w_kernel(x_ref, g_ref, part_ref, by_x_ref, out_ref, by_x_out_ref, g_v, part_v, by_x_v, g_sem, part_sem):
    rows, columns = g_ref.shape
    early = part_ref.shape[0]
    g_load = [
        pltpu.make_async_copy(g_ref.at[pl.ds(p * rows // 8, rows // 8)], g_v.at[pl.ds(p * rows // 8, rows // 8)], g_sem.at[p])
        for p in range(8)
    ]
    load = pltpu.make_async_copy(part_ref, part_v, part_sem.at[0])
    for copy in g_load:
        copy.start()
    by_x_load = pltpu.make_async_copy(by_x_ref, by_x_v, part_sem.at[2])
    for copy in g_load:
        copy.wait()
    load.start()
    by_x_load.start()

    def outer(x_tile, out_tile):
        out_tile[...] = dot(x_tile[...], g_v[...], ((0,), (0,))).astype(BF16)

    tiles = (out_ref.shape[0] - early) // BY_W_TALL

    def run(first, count):
        skip = early // BY_W_TALL + first
        pltpu.emit_pipeline(
            outer,
            grid=(count,),
            in_specs=[pl.BlockSpec((rows, BY_W_TALL), lambda j: (0, skip + j))],
            out_specs=[pl.BlockSpec((BY_W_TALL, columns), lambda j: (skip + j, 0))],
        )(x_ref, out_ref)

    run(0, tiles // 2)
    load.wait()
    store = pltpu.make_async_copy(part_v, out_ref.at[pl.ds(0, early)], part_sem.at[1])
    store.start()
    by_x_load.wait()
    by_x_store = pltpu.make_async_copy(by_x_v, by_x_out_ref, part_sem.at[3])
    by_x_store.start()
    run(tiles // 2, tiles - tiles // 2)
    store.wait()
    by_x_store.wait()


def by_w_call(xb, g, part, by_x):
    rows, depth = xb.shape
    columns = g.shape[1]
    anywhere = pl.BlockSpec(memory_space=pl.ANY)
    dma = pltpu.SemaphoreType.DMA
    return pl.pallas_call(
        by_w_kernel,
        in_specs=[anywhere] * 4,
        out_specs=[anywhere] * 2,
        out_shape=[jax.ShapeDtypeStruct((depth, columns), BF16), jax.ShapeDtypeStruct(by_x.shape, BF16)],
        scratch_shapes=[
            pltpu.VMEM((rows, columns), BF16),
            pltpu.VMEM(part.shape, BF16),
            pltpu.VMEM(by_x.shape, BF16),
            dma((8,)),
            dma((4,)),
        ],
        compiler_params=pltpu.CompilerParams(vmem_limit_bytes=VMEM_LIMIT),
        cost_estimate=pl.CostEstimate(flops=rows * depth * columns, bytes_accessed=1 << 26, transcendentals=0),
        name="by_w",
    )(xb, g, part, by_x)


def solution(mesh):
    n = mesh.shape["tp"]

    def step(x, w, label):
        me, own, columns = lax.axis_index("tp"), x.shape[0], w.shape[1]
        piece = own // PIECES
        lab = jnp.pad(label.reshape(PIECES, piece), ((0, 0), (0, 128 - piece)))
        xb, z, rel, top, inv, loss = logits_call(n, x, w, lab)
        by_x, g, part, *_ = scatter_call(n, z, w, xb.reshape(-1, xb.shape[-1]), top, inv, rel)
        by_w, by_x = by_w_call(xb.reshape(-1, xb.shape[-1]), g.reshape(-1, columns), part, by_x)
        by_device = loss.reshape(n // 2, PIECES, 2, piece).swapaxes(1, 2).reshape(n, own)
        return lax.dynamic_index_in_dim(by_device, me, 0, keepdims=False), by_x, by_w

    return jax.shard_map(
        step,
        mesh=mesh,
        in_specs=(P(("dp", "tp"), None), P(None, "tp"), P(("dp", "tp"))),
        out_specs=(P(("dp", "tp")), P(("dp", "tp"), None), P("dp", "tp")),
        check_vma=False,
    )
```
